32 devices in a mesh: vars: 16 (over z, y, x), samp: 2 (over core).
Axes of the slice: x: 2, y: 2, z: 4, core: 2. Of those that a mesh axis runs over, the one named last changes fastest.
Arguments:
- voxel_data: bfloat16 [32768, 1536], P('vars', 'samp'), may hold values from -6 to 6
- omega_blocks: float32 [256, 8, 128, 128], P('vars'), may hold values from -0.3 to 3, as said below
- block_cols: int32 [256, 8], P('vars'), may hold values from 0 to 255, as said below
Outputs:
- gradient: float32 [256, 8, 128, 128], P('vars', None, 'samp')
- omega_next: float32 [256, 8, 128, 128], P('vars', None, 'samp')
The draws below stay inside these ranges and needn't reach their ends.
Inputs may be any that keep to these rules, and one draw needn't show every extreme that they name: Block row i is held with the rows of its device. block_cols[i, 0] = i. For s >= 1, block_cols[i, s] = j is a block row of another device, and block_cols[j, s] = i. A row names no block twice. The rows of one device name at most 8 blocks of any one other device, and exactly that many for some pair. The diagonal entries of omega_blocks[i, 0] lie between 1 and 3; all other entries lie between -0.3 and 0.3.
All inputs are finite; a program needn't handle non-finite values.
Results may differ from the reference program's by a relative error of at most 0.0034.
Values may be sent and summed in bfloat16 or wider, within the bound.
No kernel may reach another device: no remote copies, remote signals or barrier semaphores. Data moves between devices by JAX's collectives and lax.ppermute only.
A program may use at most 192 MiB of HBM per device.

```python
import jax
import jax.numpy as jnp
from jax import lax

BLOCK = 128
SLOTS = 8
ROWS_DEV = 16
BLOCK_ROWS = 256
VOXELS = 32768
SAMPLES = 1536
N_VARS = 16


def draw_block_cols(key, part):
    keys = jax.random.split(jax.random.fold_in(key, 11), 4)
    peer_count = N_VARS - 1
    shuffled = jax.random.permutation(keys[0], peer_count)
    offset = jax.random.randint(keys[1], (), 0, peer_count)
    target = N_VARS // 2 - 1
    where_target = jnp.argmax((shuffled == target).astype(jnp.int32))
    order = shuffled.at[where_target].set(shuffled[offset]).at[offset].set(target)
    flips = jax.random.randint(keys[2], (SLOTS,), 0, 2)
    relabel = jax.random.permutation(keys[3], ROWS_DEV)
    undo = jnp.argsort(relabel)
    row_ids = jnp.arange(BLOCK_ROWS)
    device = row_ids // ROWS_DEV
    labels = relabel[row_ids % ROWS_DEV]
    groups = labels // 2
    positions = jnp.arange(1, SLOTS)
    serial = groups[:, None] * (SLOTS - 1) + (positions[None, :] - 1)
    masks = order[(serial + offset) % peer_count] + 1
    partner_dev = jnp.bitwise_xor(device[:, None], masks)
    partner_label = jnp.bitwise_xor(labels[:, None], flips[1:][None, :])
    columns = partner_dev * ROWS_DEV + undo[partner_label]
    return jnp.concatenate([row_ids[:, None], columns], axis=1).astype(jnp.int32)


def draw_omega_blocks(key, part):
    first, second = jax.random.split(jax.random.fold_in(key, 23))
    shape = (BLOCK_ROWS, SLOTS, BLOCK, BLOCK)
    spread = 0.05 * jax.random.truncated_normal(first, -6.0, 6.0, shape, jnp.float32)
    diagonal = jax.random.uniform(second, (BLOCK_ROWS, BLOCK), jnp.float32, 1.0, 3.0)
    identity = jnp.eye(BLOCK, dtype=jnp.float32)
    first_slot = (jnp.arange(SLOTS) == 0).astype(jnp.float32)[None, :, None, None]
    placed = first_slot * identity[None, None] * diagonal[:, None, :, None]
    return spread * (1.0 - first_slot * identity[None, None]) + placed


def steps_of(key, dims, shards, low, largest):
    def one(axis_at, parts):
        heights = jax.random.uniform(jax.random.fold_in(jax.random.fold_in(key, 6), axis_at), (parts,), jnp.float32, low / len(shards), largest / len(shards))
        return jnp.repeat(jnp.exp(heights), dims[axis_at] // parts).reshape((-1,) + (1,) * (len(dims) - axis_at - 1))

    factor_of = one(*shards[0])
    for cut in shards[1:]:
        factor_of = factor_of * one(*cut)
    return factor_of


def bell_draw(rng, shape, deviation, limit, pieces=(), held_as=jnp.bfloat16):
    entries = jax.random.normal(rng, shape, jnp.float32) * deviation
    if len(pieces) > 0:
        entries = steps_of(rng, shape, pieces, -0.22, 0.18) * entries
    return jnp.clip(entries, min=-limit, max=limit).astype(held_as)


def setup_inputs(seed: int = 0) -> dict:
    streams_of = jax.random.split(jax.random.key(seed), 4)
    return {
        "voxel_data": bell_draw(streams_of[0], (VOXELS, SAMPLES), 1.0, 6.0, ((0, 16), (1, 2))),
        "omega_blocks": draw_omega_blocks(jax.random.fold_in(streams_of[3], 71), 0),
        "block_cols": draw_block_cols(jax.random.fold_in(streams_of[3], 71), 0),
    }


STEP = 0.5
PENALTY = 0.1


def reference(voxel_data, omega_blocks, block_cols):
    block_width = omega_blocks.shape[2]
    sample_total = voxel_data.shape[1]
    panels = voxel_data.reshape(BLOCK_ROWS, block_width, sample_total)
    omega_low = omega_blocks.astype(jnp.bfloat16)

    def row_product(pair):
        blocks, columns = pair
        chosen = jnp.take(panels, columns, axis=0).astype(jnp.float32)
        summed = jnp.einsum('kab,kbn->an', blocks.astype(jnp.float32), chosen)
        rounded = lax.optimization_barrier(summed.astype(jnp.bfloat16))
        w_row = rounded.astype(jnp.float32)
        return jnp.einsum('an,kbn->kab', w_row, chosen)

    grams = lax.map(row_product, (omega_low, block_cols))
    mirror = grams[block_cols, jnp.arange(SLOTS, dtype=jnp.int32)[None, :]]
    gradient = (grams + jnp.swapaxes(mirror, 2, 3)) * (0.5 / sample_total)
    diagonal = jnp.diagonal(omega_blocks[:, 0], axis1=1, axis2=2)
    identity = jnp.eye(block_width, dtype=jnp.float32)
    gradient = gradient.at[:, 0].add(-identity[None] * (1.0 / diagonal)[:, :, None])
    trial = omega_blocks - STEP * gradient
    shrunk = jnp.sign(trial) * jnp.maximum(jnp.abs(trial) - STEP * PENALTY, 0.0)
    first_slot = (jnp.arange(SLOTS) == 0)[None, :, None, None]
    on_diagonal = jnp.logical_and(first_slot, identity[None, None] > 0.5)
    omega_next = jnp.where(on_diagonal, trial, shrunk)
    return gradient, omega_next
```

```python
import jax
import jax.numpy as jnp
from jax import lax
from jax.experimental import pallas as pl
from jax.experimental.pallas import tpu as pltpu
from jax.sharding import PartitionSpec as P


STEP = 0.5
PENALTY = 0.1


def line_length(devices):
    bits = devices.bit_length() - 1
    return 1 << -(-bits // 3)


def arrivals(place, length):
    others = [p for p in range(length) if p != place]
    outward = 1 if 2 * place < length else -1
    return sorted(others, key=lambda p: (abs(p - place), outward * (p - place)))


def select_kernel(sources, targets, capacity):
    def body(info_ref, *refs):
        ins, outs = refs[:sources], refs[sources : sources + targets]
        held, came, left = refs[sources + targets :]

        for k in range(sources):

            @pl.when(info_ref[targets * capacity] == k)
            def _(k=k):
                for t in range(targets):
                    for c in range(capacity):
                        panel = info_ref[t * capacity + c]
                        pltpu.make_async_copy(ins[k].at[panel], held.at[t, c], came.at[t]).start()

        for t in range(targets):
            pltpu.make_async_copy(held.at[t], held.at[t], came.at[t]).wait()
            pltpu.make_async_copy(held.at[t], outs[t], left.at[t]).start()
        for t in range(targets):
            pltpu.make_async_copy(held.at[t], outs[t], left.at[t]).wait()

    return body


def select_panels(info, arrays, targets, capacity):
    _, block_width, samples = arrays[0].shape
    shape = jax.ShapeDtypeStruct((capacity, block_width, samples), arrays[0].dtype)
    moved = 2 * targets * capacity * block_width * samples * 2
    return pl.pallas_call(
        select_kernel(len(arrays), targets, capacity),
        out_shape=[shape] * targets,
        in_specs=[pl.BlockSpec(memory_space=pltpu.SMEM)]
        + [pl.BlockSpec(memory_space=pl.ANY)] * len(arrays),
        out_specs=[pl.BlockSpec(memory_space=pl.ANY)] * targets,
        scratch_shapes=[
            pltpu.VMEM((targets, capacity, block_width, samples), arrays[0].dtype),
            pltpu.SemaphoreType.DMA((targets,)),
            pltpu.SemaphoreType.DMA((targets,)),
        ],
        cost_estimate=pl.CostEstimate(flops=0, transcendentals=0, bytes_accessed=moved),
        name="select_panels",
    )(info, *arrays)


def gram_kernel(layout, kslots, capacity, half_rows):
    def body(entry_ref, panel_ref, code_ref, omega_ref, own_ref, *refs):
        arrays = refs[: len(layout)]
        keep_row, keep_col, send_row, send_col, table, sem = refs[len(layout) :]
        row = pl.program_id(0)
        block_width = table.shape[1] // kslots

        def fetch(source, k, c, fixed):
            entry = entry_ref[source * capacity + c]
            i = entry // kslots
            s = entry % kslots
            panel = c if fixed else panel_ref[source * capacity + c]

            @pl.when(entry >= 0)
            def _():
                at = pl.multiple_of(s * block_width, block_width)
                pltpu.make_async_copy(
                    arrays[k].at[panel], table.at[i, pl.ds(at, block_width)], sem.at[i]
                ).start()

        @pl.when(row == 0)
        def _():
            for i in range(table.shape[0]):
                pltpu.make_async_copy(
                    own_ref.at[i], table.at[i, pl.ds(0, block_width)], sem.at[i]
                ).start()
            for k, users in enumerate(layout):
                for source, code in users:
                    if code is None:
                        for c in range(capacity):
                            fetch(source, k, c, True)
                    else:

                        @pl.when(code_ref[source] == code)
                        def _(source=source, k=k):
                            for c in range(capacity):
                                fetch(source, k, c, False)

        pltpu.make_async_copy(table.at[row], table.at[row], sem.at[row]).wait()
        panels = table[row]
        w_row = jnp.zeros((block_width, panels.shape[1]), jnp.float32)
        for s in range(kslots):
            w_row += jnp.dot(
                omega_ref[0, s].astype(jnp.bfloat16),
                panels[s * block_width : (s + 1) * block_width],
                preferred_element_type=jnp.float32,
            )
        w_row = w_row.astype(jnp.bfloat16)
        contract = (((1,), (1,)), ((), ()))
        gram = lax.dot_general(w_row, panels, contract, preferred_element_type=jnp.float32)
        flipped = lax.dot_general(panels, w_row, contract, preferred_element_type=jnp.float32)
        first = code_ref[code_ref.shape[0] - 1] == 0
        for s in range(kslots):
            part = gram[:, s * block_width : (s + 1) * block_width]
            mine = jnp.where(first, part[:half_rows], part[half_rows:])
            other = jnp.where(first, part[half_rows:], part[:half_rows])
            keep_row[0, s] = mine
            send_row[0, s] = other.astype(jnp.bfloat16)
            part = flipped[s * block_width : (s + 1) * block_width]
            mine = jnp.where(first, part[:half_rows], part[half_rows:])
            other = jnp.where(first, part[half_rows:], part[:half_rows])
            keep_col[0, s] = mine
            send_col[0, s] = other.astype(jnp.bfloat16)

    return body


def grams_of(entries, panel_ids, codes, omega_blocks, own, arrays, layout, capacity, half_rows):
    row_count, kslots, block_width, _ = omega_blocks.shape
    samples = own.shape[2]
    half = (1, kslots, half_rows, block_width)
    whole = (row_count, kslots, half_rows, block_width)
    flops = 6 * row_count * kslots * block_width * block_width * samples
    spec = pl.BlockSpec(half, lambda i, *_: (i, 0, 0, 0))
    return pl.pallas_call(
        gram_kernel(layout, kslots, capacity, half_rows),
        out_shape=[jax.ShapeDtypeStruct(whole, jnp.float32)] * 2
        + [jax.ShapeDtypeStruct(whole, jnp.bfloat16)] * 2,
        grid_spec=pltpu.PrefetchScalarGridSpec(
            num_scalar_prefetch=3,
            grid=(row_count,),
            in_specs=[pl.BlockSpec((1, kslots, block_width, block_width), lambda i, *_: (i, 0, 0, 0))]
            + [pl.BlockSpec(memory_space=pl.ANY)] * (1 + len(arrays)),
            out_specs=[spec] * 4,
            scratch_shapes=[
                pltpu.VMEM((row_count, kslots * block_width, samples), jnp.bfloat16),
                pltpu.SemaphoreType.DMA((row_count,)),
            ],
        ),
        compiler_params=pltpu.CompilerParams(
            dimension_semantics=("arbitrary",), vmem_limit_bytes=56 << 20
        ),
        cost_estimate=pl.CostEstimate(
            flops=flops, transcendentals=0, bytes_accessed=(kslots * row_count + 64) * block_width * samples * 2
        ),
        name="grams",
    )(entries, panel_ids, codes, omega_blocks, own, *arrays)


def rows_per_step(row_count):
    return 4 if row_count % 4 == 0 else 1


def outgoing_kernel(slot_ref, keep_ref, came_ref, own_ref, out_ref):
    rows, kslots = keep_ref.shape[:2]
    first = pl.program_id(0) * rows
    for r in range(rows):
        own_ref[r] = keep_ref[r, 0] + came_ref[r, 0].astype(jnp.float32)
        for s in range(1, kslots):
            summed = keep_ref[r, s] + came_ref[r, s].astype(jnp.float32)
            out_ref[slot_ref[(first + r) * kslots + s]] = summed.astype(jnp.bfloat16)


def outgoing_blocks(slots, keep_col, came_col, slot_count):
    row_count, kslots, half_rows, block_width = keep_col.shape
    rows = rows_per_step(row_count)
    spec = pl.BlockSpec((rows, kslots, half_rows, block_width), lambda i, *_: (i, 0, 0, 0))
    return pl.pallas_call(
        outgoing_kernel,
        out_shape=[
            jax.ShapeDtypeStruct((row_count, half_rows, block_width), jnp.float32),
            jax.ShapeDtypeStruct((slot_count, half_rows, block_width), jnp.bfloat16),
        ],
        grid_spec=pltpu.PrefetchScalarGridSpec(
            num_scalar_prefetch=1,
            grid=(row_count // rows,),
            in_specs=[spec, spec],
            out_specs=[
                pl.BlockSpec((rows, half_rows, block_width), lambda i, *_: (i, 0, 0)),
                pl.BlockSpec((slot_count, half_rows, block_width), lambda i, *_: (0, 0, 0)),
            ],
        ),
        compiler_params=pltpu.CompilerParams(dimension_semantics=("arbitrary",)),
        name="outgoing",
    )(slots, keep_col, came_col)


def final_kernel(scale):
    def body(slot_ref, half_ref, keep_ref, came_ref, own_ref, mirror_ref, omega_ref, grad_ref, next_ref):
        rows, kslots, half_rows, block_width = keep_ref.shape
        first = pl.program_id(0) * rows
        start = half_ref[0] * half_rows
        row_ids = lax.broadcasted_iota(jnp.int32, (half_rows, block_width), 0) + start
        col_ids = lax.broadcasted_iota(jnp.int32, (half_rows, block_width), 1)
        on_diagonal = row_ids == col_ids
        for r in range(rows):
            for s in range(kslots):
                omega = omega_ref[r, s]
                if s == 0:
                    mirror = own_ref[r]
                else:
                    mirror = mirror_ref[slot_ref[(first + r) * kslots + s]].astype(jnp.float32)
                gradient = (keep_ref[r, s] + came_ref[r, s].astype(jnp.float32) + mirror) * scale
                if s == 0:
                    inverse = 1.0 / jnp.where(on_diagonal, omega, 1.0)
                    gradient = gradient - jnp.where(on_diagonal, inverse, 0.0)
                trial = omega - STEP * gradient
                size = jnp.maximum(jnp.abs(trial) - STEP * PENALTY, 0.0)
                shrunk = jnp.where(trial < 0.0, -size, size)
                if s == 0:
                    shrunk = jnp.where(on_diagonal, trial, shrunk)
                grad_ref[r, s] = gradient
                next_ref[r, s] = shrunk

    return body


def final_step(slots, sample_part, keep_row, came_row, own_col, incoming, omega_blocks, scale):
    row_count, kslots, half_rows, block_width = keep_row.shape
    rows = rows_per_step(row_count)
    spec = pl.BlockSpec((rows, kslots, half_rows, block_width), lambda i, *_: (i, 0, 0, 0))
    shape = jax.ShapeDtypeStruct(keep_row.shape, jnp.float32)
    return pl.pallas_call(
        final_kernel(scale),
        out_shape=[shape, shape],
        grid_spec=pltpu.PrefetchScalarGridSpec(
            num_scalar_prefetch=2,
            grid=(row_count // rows,),
            in_specs=[
                spec,
                spec,
                pl.BlockSpec((rows, half_rows, block_width), lambda i, *_: (i, 0, 0)),
                pl.BlockSpec(incoming.shape, lambda i, *_: (0, 0, 0)),
                pl.BlockSpec(
                    (rows, kslots, half_rows, block_width),
                    lambda i, slot, half: (i, 0, half[0], 0),
                ),
            ],
            out_specs=[spec, spec],
        ),
        compiler_params=pltpu.CompilerParams(dimension_semantics=("arbitrary",)),
        name="final_step",
    )(slots, sample_part.reshape(1), keep_row, came_row, own_col, incoming, omega_blocks)


def ranks_among(same, keys):
    return jnp.sum((same & (keys[..., None, :] < keys[..., :, None])).astype(jnp.int32), axis=-1)


def step_on_device(voxel_data, omega_blocks, block_cols):
    row_count, kslots, block_width, _ = omega_blocks.shape
    devices = lax.axis_size("vars")
    samp_count = lax.axis_size("samp")
    me = lax.axis_index("vars")
    sample_part = lax.axis_index("samp")
    half_rows = block_width // samp_count
    samples = voxel_data.shape[1]
    total_samples = samples * samp_count
    capacity = 2 * ((row_count // 2 * (kslots - 1) + devices - 2) // (devices - 1))
    entries = row_count * kslots
    length = line_length(devices)
    plane = devices // length
    place, seat = me // plane, me % plane
    panels = voxel_data.reshape(row_count, block_width, samples)

    def along(array, step):
        pairs = [
            (p * plane + b, (p + step) * plane + b)
            for p in range(length)
            if 0 <= p + step < length
            for b in range(plane)
        ]
        return lax.ppermute(array, "vars", pairs)

    def across(array, mask):
        pairs = [(p * plane + b, p * plane + (b ^ mask)) for p in range(length) for b in range(plane)]
        return lax.ppermute(array, "vars", pairs)

    order = [[p] + arrivals(p, length) for p in range(length)]
    offsets = [[order[p][m] - p for p in range(length)] for m in range(length)]
    sources = jnp.array(order, jnp.int32)[place]

    all_cols = lax.all_gather(block_cols, "vars", axis=0, tiled=False)
    panels, all_cols = lax.optimization_barrier((panels, all_cols))

    source_cols = all_cols[sources * plane + seat].reshape(length, entries)
    entry_ids = jnp.arange(entries, dtype=jnp.int32)
    remote = entry_ids % kslots != 0
    targets = place * plane + (seat ^ jnp.arange(1, plane, dtype=jnp.int32))
    hits = (source_cols[:, None, :] // row_count == targets[None, :, None]) & remote
    before = ranks_among(hits[:, :, None, :], jnp.broadcast_to(entry_ids, hits.shape))
    chosen = hits[:, :, None, :] & (
        before[:, :, None, :] == jnp.arange(capacity, dtype=jnp.int32)[None, None, :, None]
    )
    picks = jnp.sum(jnp.where(chosen, entry_ids // kslots, 0), axis=-1).reshape(length, -1)

    flat_cols = block_cols.reshape(entries)
    owners = flat_cols // row_count
    same_peer = (owners[:, None] == owners[None, :]) & remote[:, None] & remote[None, :]
    sort_keys = flat_cols * kslots + entry_ids % kslots
    entry_rank = ranks_among(same_peer, entry_ids)
    key_rank = ranks_among(same_peer, sort_keys)
    mirror_in = owners * capacity + entry_rank
    mirror_out = owners * capacity + key_rank
    peers = (
        sources[:, None] * plane + (seat ^ jnp.arange(plane, dtype=jnp.int32))[None, :]
    ).reshape(-1)
    wanted = (
        remote
        & (owners == peers[:, None])[:, None, :]
        & (key_rank == jnp.arange(capacity, dtype=jnp.int32)[:, None])[None]
    )
    entry_table = (jnp.sum(jnp.where(wanted, entry_ids + 1, 0), axis=-1) - 1).reshape(-1)
    panel_table = jnp.sum(jnp.where(wanted, flat_cols % row_count, 0), axis=-1).reshape(-1)

    came = {0: panels}
    received = []
    codes = []
    for m in range(length):
        if m > 0:
            for step in (-1, 1):
                came[step * m] = along(came[step * (m - 1)], -step)
        options = sorted(set(offsets[m]))
        code = jnp.array([options.index(o) for o in offsets[m]], jnp.int32)[place]
        codes.append((options, code))
        info = jnp.concatenate([picks[m], code[None]])
        sent = select_panels(info, [came[o] for o in options], plane - 1, capacity)
        received.append([across(block, mask + 1) for mask, block in enumerate(sent)])

    arrays, layout, code_values = [], [], [jnp.int32(0)] * (length * plane + 1)
    line_users = {}
    for m in range(length):
        for mask in range(1, plane):
            arrays.append(received[m][mask - 1])
            layout.append([(m * plane + mask, None)])
        if m > 0:
            options, code = codes[m]
            code_values[m * plane] = code
            for number, option in enumerate(options):
                line_users.setdefault(option, []).append((m * plane, number))
    for option in sorted(line_users):
        arrays.append(came[option])
        layout.append(line_users[option])
    code_values[-1] = sample_part
    keep_row, keep_col, send_row, send_col = grams_of(
        entry_table,
        panel_table,
        jnp.stack(code_values),
        omega_blocks,
        panels,
        arrays,
        layout,
        capacity,
        half_rows,
    )

    swap = [(k, samp_count - 1 - k) for k in range(samp_count)]
    came_col = lax.ppermute(send_col, "samp", swap)
    came_row = lax.ppermute(send_row, "samp", swap)
    own_col, outgoing = outgoing_blocks(mirror_out, keep_col, came_col, devices * capacity)
    incoming = lax.all_to_all(
        outgoing.reshape(devices, capacity, half_rows, block_width),
        "vars",
        split_axis=0,
        concat_axis=0,
        tiled=True,
    ).reshape(devices * capacity, half_rows, block_width)
    return tuple(
        final_step(
            mirror_in,
            sample_part,
            keep_row,
            came_row,
            own_col,
            incoming,
            omega_blocks,
            0.5 / total_samples,
        )
    )


def solution(mesh):
    in_specs = (P("vars", "samp"), P("vars", None, None, None), P("vars", None))
    out_specs = (P("vars", None, "samp", None), P("vars", None, "samp", None))
    return jax.shard_map(
        step_on_device, mesh=mesh, in_specs=in_specs, out_specs=out_specs, check_vma=False
    )
```

```python
import jax
import jax.numpy as jnp
from jax import lax
from jax.experimental import pallas as pl
from jax.experimental.pallas import tpu as pltpu
from jax.sharding import PartitionSpec as P


STEP = 0.5
PENALTY = 0.1


def line_length(devices):
    bits = devices.bit_length() - 1
    return 1 << -(-bits // 3)


def arrivals(place, length):
    others = [p for p in range(length) if p != place]
    outward = 1 if 2 * place < length else -1
    return sorted(others, key=lambda p: (abs(p - place), outward * (p - place)))


def select_kernel(phase, sources, targets, capacity):
    def body(info_ref, *refs):
        cols, ins = refs[:sources], refs[sources : 2 * sources]
        outs = refs[2 * sources : 2 * sources + targets]
        held, counts, came, left = refs[2 * sources + targets :]
        row_count, kslots = cols[0].shape
        plane = targets + 1
        place, seat = info_ref[0], info_ref[1]
        for t in range(plane):
            counts[t] = 0

        for k in range(sources):

            @pl.when(info_ref[2 + phase] == k)
            def _(k=k):
                def row_step(i, carry):
                    for s in range(1, kslots):
                        owner = cols[k][i, s] // row_count
                        mask = (owner % plane) ^ seat

                        @pl.when((owner // plane == place) & (mask > 0))
                        def _():
                            c = counts[mask]
                            counts[mask] = c + 1
                            pltpu.make_async_copy(
                                ins[k].at[i], held.at[mask - 1, c], came.at[mask - 1]
                            ).start()

                    return carry

                lax.fori_loop(0, row_count, row_step, 0)

        for t in range(targets):

            def fill(c, carry, t=t):
                pltpu.make_async_copy(ins[0].at[0], held.at[t, c], came.at[t]).start()
                return carry

            lax.fori_loop(counts[t + 1], capacity, fill, 0)
        for t in range(targets):
            pltpu.make_async_copy(held.at[t], held.at[t], came.at[t]).wait()
            pltpu.make_async_copy(held.at[t], outs[t], left.at[t]).start()
        for t in range(targets):
            pltpu.make_async_copy(held.at[t], outs[t], left.at[t]).wait()

    return body


def select_panels(phase, info, cols, arrays, targets, capacity):
    _, block_width, samples = arrays[0].shape
    shape = jax.ShapeDtypeStruct((capacity, block_width, samples), arrays[0].dtype)
    moved = 2 * targets * capacity * block_width * samples * 2
    return pl.pallas_call(
        select_kernel(phase, len(arrays), targets, capacity),
        out_shape=[shape] * targets,
        in_specs=[pl.BlockSpec(memory_space=pltpu.SMEM)] * (1 + len(cols))
        + [pl.BlockSpec(memory_space=pl.ANY)] * len(arrays),
        out_specs=[pl.BlockSpec(memory_space=pl.ANY)] * targets,
        scratch_shapes=[
            pltpu.VMEM((targets, capacity, block_width, samples), arrays[0].dtype),
            pltpu.SMEM((targets + 1,), jnp.int32),
            pltpu.SemaphoreType.DMA((targets,)),
            pltpu.SemaphoreType.DMA((targets,)),
        ],
        cost_estimate=pl.CostEstimate(flops=0, transcendentals=0, bytes_accessed=moved),
        name="select_panels",
    )(info, *cols, *arrays)


def gather_kernel(layout, kslots, capacity):
    def body(entry_ref, panel_ref, code_ref, late_ref, omega_ref, own_ref, *refs):
        arrays = refs[: len(layout)]
        part_ref, rows_ref, table, sem = refs[len(layout) :]
        row = pl.program_id(0)
        block_width = table.shape[1] // kslots

        def place(panel, i, s):
            at = pl.multiple_of(s * block_width, block_width)
            pltpu.make_async_copy(panel, table.at[i, pl.ds(at, block_width)], sem.at[i]).start()

        def fetch(source, k, c, fixed):
            entry = entry_ref[source * capacity + c]
            panel = c if fixed else panel_ref[source * capacity + c]

            @pl.when(entry >= 0)
            def _():
                place(arrays[k].at[panel], entry // kslots, entry % kslots)

        @pl.when(row == 0)
        def _():
            for i in range(table.shape[0]):
                place(own_ref.at[i], i, 0)
            for i in range(table.shape[0]):
                for s in range(1, kslots):

                    @pl.when(late_ref[i * kslots + s] >= 0)
                    def _(i=i, s=s):
                        place(own_ref.at[i], i, s)

            for k, users in enumerate(layout):
                for source, code in users:
                    if code is None:
                        for c in range(capacity):
                            fetch(source, k, c, True)
                    else:

                        @pl.when(code_ref[source] == code)
                        def _(source=source, k=k):
                            for c in range(capacity):
                                fetch(source, k, c, False)

        pltpu.make_async_copy(table.at[row], table.at[row], sem.at[row]).wait()
        rows_ref[0] = table[row]
        part = jnp.zeros(part_ref.shape[1:], jnp.float32)
        for s in range(kslots):
            omega = omega_ref[0, s]
            if s > 0:
                omega = jnp.where(late_ref[row * kslots + s] >= 0, 0.0, omega)
            part += jnp.dot(
                omega.astype(jnp.bfloat16),
                table[row, s * block_width : (s + 1) * block_width],
                preferred_element_type=jnp.float32,
            )
        part_ref[0] = part

    return body


def gather_early(entries, panel_ids, codes, late, omega_blocks, own, arrays, layout, capacity):
    row_count, kslots, block_width, _ = omega_blocks.shape
    samples = own.shape[2]
    flops = 2 * row_count * kslots * block_width * block_width * samples
    return pl.pallas_call(
        gather_kernel(layout, kslots, capacity),
        out_shape=[
            jax.ShapeDtypeStruct((row_count, block_width, samples), jnp.float32),
            jax.ShapeDtypeStruct((row_count, kslots * block_width, samples), jnp.bfloat16),
        ],
        grid_spec=pltpu.PrefetchScalarGridSpec(
            num_scalar_prefetch=4,
            grid=(row_count,),
            in_specs=[pl.BlockSpec((1, kslots, block_width, block_width), lambda i, *_: (i, 0, 0, 0))]
            + [pl.BlockSpec(memory_space=pl.ANY)] * (1 + len(arrays)),
            out_specs=[
                pl.BlockSpec((1, block_width, samples), lambda i, *_: (i, 0, 0)),
                pl.BlockSpec((1, kslots * block_width, samples), lambda i, *_: (i, 0, 0)),
            ],
            scratch_shapes=[
                pltpu.VMEM((row_count, kslots * block_width, samples), jnp.bfloat16),
                pltpu.SemaphoreType.DMA((row_count,)),
            ],
        ),
        compiler_params=pltpu.CompilerParams(
            dimension_semantics=("arbitrary",), vmem_limit_bytes=56 << 20
        ),
        cost_estimate=pl.CostEstimate(
            flops=flops,
            transcendentals=0,
            bytes_accessed=2 * kslots * row_count * block_width * samples * 2,
        ),
        name="gather_early",
    )(entries, panel_ids, codes, late, omega_blocks, own, *arrays)


def gram_kernel(line_count, kslots, capacity, half_rows):
    def body(panel_ref, code_ref, late_ref, omega_ref, part_ref, rows_ref, *refs):
        lines = refs[:line_count]
        came = refs[line_count:-7]
        grams_ref, send_ref, table, held, w_row, sem, held_sem = refs[-7:]
        row = pl.program_id(0)
        block_width = w_row.shape[0]

        @pl.when(row == 0)
        def _():
            for k in range(line_count):

                @pl.when(code_ref[0] == k)
                def _(k=k):
                    for c in range(capacity):
                        pltpu.make_async_copy(
                            lines[k].at[panel_ref[c]], held.at[c], held_sem.at[0]
                        ).start()

            for mask, block in enumerate(came):
                at = pl.ds((mask + 1) * capacity, capacity)
                pltpu.make_async_copy(block, held.at[at], held_sem.at[0]).start()
            for i in range(table.shape[0]):
                pltpu.make_async_copy(rows_ref.at[i], table.at[i], sem.at[i]).start()
            pltpu.make_async_copy(held, held, held_sem.at[0]).wait()

        w_row[...] = part_ref[0]
        pltpu.make_async_copy(table.at[row], table.at[row], sem.at[row]).wait()
        for s in range(1, kslots):
            late = late_ref[row * kslots + s]

            @pl.when(late >= 0)
            def _(s=s, late=late):
                panel = held[late]
                table[row, s * block_width : (s + 1) * block_width] = panel
                w_row[...] += jnp.dot(
                    omega_ref[0, s].astype(jnp.bfloat16),
                    panel,
                    preferred_element_type=jnp.float32,
                )

        flipped = lax.dot_general(
            table[row],
            w_row[...].astype(jnp.bfloat16),
            (((1,), (1,)), ((), ())),
            preferred_element_type=jnp.float32,
        )
        first = code_ref[1] == 0
        for s in range(kslots):
            block = flipped[s * block_width : (s + 1) * block_width]
            grams_ref[0, s] = block
            send_ref[0, s] = jnp.where(first, block[half_rows:], block[:half_rows]).astype(
                jnp.bfloat16
            )

    return body


def grams_of(panel_ids, codes, late, omega_blocks, part, rows, lines, came, capacity, half_rows):
    row_count, kslots, block_width, _ = omega_blocks.shape
    samples = part.shape[2]
    flops = 2 * row_count * kslots * block_width * block_width * samples
    return pl.pallas_call(
        gram_kernel(len(lines), kslots, capacity, half_rows),
        out_shape=[
            jax.ShapeDtypeStruct(omega_blocks.shape, jnp.float32),
            jax.ShapeDtypeStruct((row_count, kslots, half_rows, block_width), jnp.bfloat16),
        ],
        grid_spec=pltpu.PrefetchScalarGridSpec(
            num_scalar_prefetch=3,
            grid=(row_count,),
            in_specs=[
                pl.BlockSpec((1, kslots, block_width, block_width), lambda i, *_: (i, 0, 0, 0)),
                pl.BlockSpec((1, block_width, samples), lambda i, *_: (i, 0, 0)),
            ]
            + [pl.BlockSpec(memory_space=pl.ANY)] * (1 + len(lines) + len(came)),
            out_specs=[
                pl.BlockSpec((1, kslots, block_width, block_width), lambda i, *_: (i, 0, 0, 0)),
                pl.BlockSpec((1, kslots, half_rows, block_width), lambda i, *_: (i, 0, 0, 0)),
            ],
            scratch_shapes=[
                pltpu.VMEM((row_count, kslots * block_width, samples), jnp.bfloat16),
                pltpu.VMEM(((1 + len(came)) * capacity, block_width, samples), jnp.bfloat16),
                pltpu.VMEM((block_width, samples), jnp.float32),
                pltpu.SemaphoreType.DMA((row_count,)),
                pltpu.SemaphoreType.DMA((1,)),
            ],
        ),
        compiler_params=pltpu.CompilerParams(
            dimension_semantics=("arbitrary",), vmem_limit_bytes=56 << 20
        ),
        cost_estimate=pl.CostEstimate(
            flops=flops,
            transcendentals=0,
            bytes_accessed=(kslots + 4) * row_count * block_width * samples * 2,
        ),
        name="grams",
    )(panel_ids, codes, late, omega_blocks, part, rows, *lines, *came)


def turn_kernel(part_ref, grams_ref, keep_ref, send_ref):
    first = part_ref[0] == 0
    half_rows = keep_ref.shape[2]
    for s in range(keep_ref.shape[1]):
        turned = grams_ref[0, s].T
        low, high = turned[:half_rows], turned[half_rows:]
        keep_ref[0, s] = jnp.where(first, low, high)
        send_ref[0, s] = jnp.where(first, high, low).astype(jnp.bfloat16)


def turned_halves(sample_part, grams, half_rows):
    row_count, kslots, block_width, _ = grams.shape
    spec = pl.BlockSpec((1, kslots, half_rows, block_width), lambda i, *_: (i, 0, 0, 0))
    shape = (row_count, kslots, half_rows, block_width)
    return pl.pallas_call(
        turn_kernel,
        out_shape=[jax.ShapeDtypeStruct(shape, jnp.float32), jax.ShapeDtypeStruct(shape, jnp.bfloat16)],
        grid_spec=pltpu.PrefetchScalarGridSpec(
            num_scalar_prefetch=1,
            grid=(row_count,),
            in_specs=[pl.BlockSpec((1,) + grams.shape[1:], lambda i, *_: (i, 0, 0, 0))],
            out_specs=[spec, spec],
        ),
        compiler_params=pltpu.CompilerParams(dimension_semantics=("arbitrary",)),
        name="turn",
    )(sample_part.reshape(1), grams)


def rows_per_step(row_count):
    return 4 if row_count % 4 == 0 else 1


def outgoing_kernel(slot_ref, half_ref, keep_ref, came_ref, own_ref, out_ref):
    rows, kslots = keep_ref.shape[:2]
    first = pl.program_id(0) * rows
    for r in range(rows):
        own_ref[r] = keep_ref[r, 0] + came_ref[r, 0].astype(jnp.float32)
        for s in range(1, kslots):
            summed = keep_ref[r, s] + came_ref[r, s].astype(jnp.float32)
            out_ref[slot_ref[(first + r) * kslots + s]] = summed.astype(jnp.bfloat16)


def outgoing_blocks(slots, sample_part, grams, came_col, slot_count):
    row_count, kslots, half_rows, block_width = came_col.shape
    rows = rows_per_step(row_count)
    spec = pl.BlockSpec((rows, kslots, half_rows, block_width), lambda i, *_: (i, 0, 0, 0))
    return pl.pallas_call(
        outgoing_kernel,
        out_shape=[
            jax.ShapeDtypeStruct((row_count, half_rows, block_width), jnp.float32),
            jax.ShapeDtypeStruct((slot_count, half_rows, block_width), jnp.bfloat16),
        ],
        grid_spec=pltpu.PrefetchScalarGridSpec(
            num_scalar_prefetch=2,
            grid=(row_count // rows,),
            in_specs=[
                pl.BlockSpec(
                    (rows, kslots, half_rows, block_width),
                    lambda i, slot, half: (i, 0, half[0], 0),
                ),
                spec,
            ],
            out_specs=[
                pl.BlockSpec((rows, half_rows, block_width), lambda i, *_: (i, 0, 0)),
                pl.BlockSpec((slot_count, half_rows, block_width), lambda i, *_: (0, 0, 0)),
            ],
        ),
        compiler_params=pltpu.CompilerParams(dimension_semantics=("arbitrary",)),
        name="outgoing",
    )(slots, sample_part.reshape(1), grams, came_col)


def final_kernel(scale):
    def body(slot_ref, half_ref, keep_ref, came_ref, own_ref, mirror_ref, omega_ref, grad_ref, next_ref):
        rows, kslots, half_rows, block_width = keep_ref.shape
        first = pl.program_id(0) * rows
        start = half_ref[0] * half_rows
        row_ids = lax.broadcasted_iota(jnp.int32, (half_rows, block_width), 0) + start
        col_ids = lax.broadcasted_iota(jnp.int32, (half_rows, block_width), 1)
        on_diagonal = row_ids == col_ids
        for r in range(rows):
            for s in range(kslots):
                omega = omega_ref[r, s]
                if s == 0:
                    mirror = own_ref[r]
                else:
                    mirror = mirror_ref[slot_ref[(first + r) * kslots + s]].astype(jnp.float32)
                gradient = (keep_ref[r, s] + came_ref[r, s].astype(jnp.float32) + mirror) * scale
                if s == 0:
                    inverse = 1.0 / jnp.where(on_diagonal, omega, 1.0)
                    gradient = gradient - jnp.where(on_diagonal, inverse, 0.0)
                trial = omega - STEP * gradient
                size = jnp.maximum(jnp.abs(trial) - STEP * PENALTY, 0.0)
                shrunk = jnp.where(trial < 0.0, -size, size)
                if s == 0:
                    shrunk = jnp.where(on_diagonal, trial, shrunk)
                grad_ref[r, s] = gradient
                next_ref[r, s] = shrunk

    return body


def final_step(slots, sample_part, keep_row, came_row, own_col, incoming, omega_blocks, scale):
    row_count, kslots, half_rows, block_width = keep_row.shape
    rows = rows_per_step(row_count)
    spec = pl.BlockSpec((rows, kslots, half_rows, block_width), lambda i, *_: (i, 0, 0, 0))
    shape = jax.ShapeDtypeStruct(keep_row.shape, jnp.float32)
    return pl.pallas_call(
        final_kernel(scale),
        out_shape=[shape, shape],
        grid_spec=pltpu.PrefetchScalarGridSpec(
            num_scalar_prefetch=2,
            grid=(row_count // rows,),
            in_specs=[
                spec,
                spec,
                pl.BlockSpec((rows, half_rows, block_width), lambda i, *_: (i, 0, 0)),
                pl.BlockSpec(incoming.shape, lambda i, *_: (0, 0, 0)),
                pl.BlockSpec(
                    (rows, kslots, half_rows, block_width),
                    lambda i, slot, half: (i, 0, half[0], 0),
                ),
            ],
            out_specs=[spec, spec],
        ),
        compiler_params=pltpu.CompilerParams(dimension_semantics=("arbitrary",)),
        name="final_step",
    )(slots, sample_part.reshape(1), keep_row, came_row, own_col, incoming, omega_blocks)


def ranks_among(same, keys):
    return jnp.sum((same & (keys[..., None, :] < keys[..., :, None])).astype(jnp.int32), axis=-1)


def step_on_device(voxel_data, omega_blocks, block_cols):
    row_count, kslots, block_width, _ = omega_blocks.shape
    devices = lax.axis_size("vars")
    samp_count = lax.axis_size("samp")
    me = lax.axis_index("vars")
    sample_part = lax.axis_index("samp")
    half_rows = block_width // samp_count
    samples = voxel_data.shape[1]
    total_samples = samples * samp_count
    capacity = 2 * ((row_count // 2 * (kslots - 1) + devices - 2) // (devices - 1))
    entries = row_count * kslots
    length = line_length(devices)
    plane = devices // length
    place, seat = me // plane, me % plane
    panels = voxel_data.reshape(row_count, block_width, samples)

    def along(array, step):
        pairs = [
            (p * plane + b, (p + step) * plane + b)
            for p in range(length)
            if 0 <= p + step < length
            for b in range(plane)
        ]
        return lax.ppermute(array, "vars", pairs)

    def across(array, mask):
        pairs = [(p * plane + b, p * plane + (b ^ mask)) for p in range(length) for b in range(plane)]
        return lax.ppermute(array, "vars", pairs)

    order = [[p] + arrivals(p, length) for p in range(length)]
    offsets = [[order[p][m] - p for p in range(length)] for m in range(length)]
    choices = [sorted(set(offsets[m])) for m in range(length)]
    sources = jnp.array(order, jnp.int32)[place]
    facts = [
        [p, b] + [choices[m].index(offsets[m][p]) for m in range(length)]
        for p in range(length)
        for b in range(plane)
    ]
    info = lax.dynamic_slice_in_dim(jnp.array(facts, jnp.int32), me, 1, 0)[0]

    came_cols = {0: block_cols}
    for m in range(1, length):
        for step in (-1, 1):
            came_cols[step * m] = along(came_cols[step * (m - 1)], -step)

    entry_ids = jnp.arange(entries, dtype=jnp.int32)
    remote = entry_ids % kslots != 0

    flat_cols = block_cols.reshape(entries)
    owners = flat_cols // row_count
    same_peer = (owners[:, None] == owners[None, :]) & remote[:, None] & remote[None, :]
    sort_keys = flat_cols * kslots + entry_ids % kslots
    entry_rank = ranks_among(same_peer, entry_ids)
    key_rank = ranks_among(same_peer, sort_keys)
    mirror_in = owners * capacity + entry_rank
    mirror_out = owners * capacity + key_rank
    peers = (
        sources[:, None] * plane + (seat ^ jnp.arange(plane, dtype=jnp.int32))[None, :]
    ).reshape(-1)
    wanted = (
        remote
        & (owners == peers[:, None])[:, None, :]
        & (key_rank == jnp.arange(capacity, dtype=jnp.int32)[:, None])[None]
    )
    entry_table = (jnp.sum(jnp.where(wanted, entry_ids + 1, 0), axis=-1) - 1).reshape(-1)
    panel_table = jnp.sum(jnp.where(wanted, flat_cols % row_count, 0), axis=-1).reshape(-1)

    late_hit = remote & (owners // plane == sources[-1])
    late = jnp.where(late_hit, ((owners % plane) ^ seat) * capacity + key_rank, -1)

    came = {0: panels}
    received = []
    for m in range(length):
        if m > 0:
            for step in (-1, 1):
                came[step * m] = along(came[step * (m - 1)], -step)
        sent = select_panels(
            m,
            info,
            [came_cols[o] for o in choices[m]],
            [came[o] for o in choices[m]],
            plane - 1,
            capacity,
        )
        received.append([across(block, mask + 1) for mask, block in enumerate(sent)])

    last = length - 1
    arrays, layout, line_users = [], [], {}
    code_values = [jnp.int32(0)] * (last * plane)
    for m in range(last):
        for mask in range(1, plane):
            arrays.append(received[m][mask - 1])
            layout.append([(m * plane + mask, None)])
        if m > 0:
            code_values[m * plane] = info[2 + m]
            for number, option in enumerate(choices[m]):
                line_users.setdefault(option, []).append((m * plane, number))
    for option in sorted(line_users):
        arrays.append(came[option])
        layout.append(line_users[option])
    early = last * plane * capacity
    part, rows = gather_early(
        entry_table[:early],
        panel_table[:early],
        jnp.stack(code_values),
        late,
        omega_blocks,
        panels,
        arrays,
        layout,
        capacity,
    )
    grams, send_col = grams_of(
        panel_table[early : early + capacity],
        jnp.stack([info[2 + last], sample_part]),
        late,
        omega_blocks,
        part,
        rows,
        [came[o] for o in choices[last]],
        received[last],
        capacity,
        half_rows,
    )

    swap = [(k, samp_count - 1 - k) for k in range(samp_count)]
    came_col = lax.ppermute(send_col, "samp", swap)
    own_col, outgoing = outgoing_blocks(
        mirror_out, sample_part, grams, came_col, devices * capacity
    )
    outgoing, grams = lax.optimization_barrier((outgoing, grams))
    incoming = lax.all_to_all(
        outgoing.reshape(devices, capacity, half_rows, block_width),
        "vars",
        split_axis=0,
        concat_axis=0,
        tiled=True,
    ).reshape(devices * capacity, half_rows, block_width)
    keep_row, send_row = turned_halves(sample_part, grams, half_rows)
    came_row = lax.ppermute(send_row, "samp", swap)
    return tuple(
        final_step(
            mirror_in,
            sample_part,
            keep_row,
            came_row,
            own_col,
            incoming,
            omega_blocks,
            0.5 / total_samples,
        )
    )


def solution(mesh):
    in_specs = (P("vars", "samp"), P("vars", None, None, None), P("vars", None))
    out_specs = (P("vars", None, "samp", None), P("vars", None, "samp", None))
    return jax.shard_map(
        step_on_device, mesh=mesh, in_specs=in_specs, out_specs=out_specs, check_vma=False
    )
```

```python
import jax
import jax.numpy as jnp
from jax import lax
from jax.experimental import pallas as pl
from jax.experimental.pallas import tpu as pltpu
from jax.sharding import PartitionSpec as P


STEP = 0.5
PENALTY = 0.1


def line_length(devices):
    bits = devices.bit_length() - 1
    return 1 << -(-bits // 3)


def arrivals(place, length):
    others = [p for p in range(length) if p != place]
    outward = 1 if 2 * place < length else -1
    return sorted(others, key=lambda p: (abs(p - place), outward * (p - place)))


def select_kernel(phase, sources, targets, capacity):
    def body(info_ref, *refs):
        cols, ins = refs[:sources], refs[sources : 2 * sources]
        outs = refs[2 * sources : 2 * sources + targets]
        held, counts, came, left = refs[2 * sources + targets :]
        row_count, kslots = cols[0].shape
        plane = targets + 1
        place, seat = info_ref[0], info_ref[1]
        for t in range(plane):
            counts[t] = 0

        for k in range(sources):

            @pl.when(info_ref[2 + phase] == k)
            def _(k=k):
                def row_step(i, carry):
                    for s in range(1, kslots):
                        owner = cols[k][i, s] // row_count
                        mask = (owner % plane) ^ seat

                        @pl.when((owner // plane == place) & (mask > 0))
                        def _():
                            c = counts[mask]
                            counts[mask] = c + 1
                            pltpu.make_async_copy(
                                ins[k].at[i], held.at[mask - 1, c], came.at[mask - 1]
                            ).start()

                    return carry

                lax.fori_loop(0, row_count, row_step, 0)

        for t in range(targets):

            def fill(c, carry, t=t):
                pltpu.make_async_copy(ins[0].at[0], held.at[t, c], came.at[t]).start()
                return carry

            lax.fori_loop(counts[t + 1], capacity, fill, 0)
        for t in range(targets):
            pltpu.make_async_copy(held.at[t], held.at[t], came.at[t]).wait()
            pltpu.make_async_copy(held.at[t], outs[t], left.at[t]).start()
        for t in range(targets):
            pltpu.make_async_copy(held.at[t], outs[t], left.at[t]).wait()

    return body


def select_panels(phase, info, cols, arrays, targets, capacity):
    _, block_width, samples = arrays[0].shape
    shape = jax.ShapeDtypeStruct((capacity, block_width, samples), arrays[0].dtype)
    moved = 2 * targets * capacity * block_width * samples * 2
    return pl.pallas_call(
        select_kernel(phase, len(arrays), targets, capacity),
        out_shape=[shape] * targets,
        in_specs=[pl.BlockSpec(memory_space=pltpu.SMEM)] * (1 + len(cols))
        + [pl.BlockSpec(memory_space=pl.ANY)] * len(arrays),
        out_specs=[pl.BlockSpec(memory_space=pl.ANY)] * targets,
        scratch_shapes=[
            pltpu.VMEM((targets, capacity, block_width, samples), arrays[0].dtype),
            pltpu.SMEM((targets + 1,), jnp.int32),
            pltpu.SemaphoreType.DMA((targets,)),
            pltpu.SemaphoreType.DMA((targets,)),
        ],
        cost_estimate=pl.CostEstimate(flops=0, transcendentals=0, bytes_accessed=moved),
        name="select_panels",
    )(info, *cols, *arrays)


def gather_kernel(layout, kslots, capacity):
    def body(entry_ref, panel_ref, code_ref, late_ref, omega_ref, own_ref, *refs):
        arrays = refs[: len(layout)]
        part_ref, rows_ref, omega_late, table, sem = refs[len(layout) :]
        row = pl.program_id(0)
        block_width = table.shape[1] // kslots

        def place(panel, i, s):
            at = pl.multiple_of(s * block_width, block_width)
            pltpu.make_async_copy(panel, table.at[i, pl.ds(at, block_width)], sem.at[i]).start()

        def fetch(source, k, c, fixed):
            entry = entry_ref[source * capacity + c]
            panel = c if fixed else panel_ref[source * capacity + c]

            @pl.when(entry >= 0)
            def _():
                place(arrays[k].at[panel], entry // kslots, entry % kslots)

        @pl.when(row == 0)
        def _():
            for i in range(table.shape[0]):
                place(own_ref.at[i], i, 0)
            for i in range(table.shape[0]):
                for s in range(1, kslots):

                    @pl.when(late_ref[i * kslots + s] >= 0)
                    def _(i=i, s=s):
                        place(own_ref.at[i], i, s)

            for k, users in enumerate(layout):
                for source, code in users:
                    if code is None:
                        for c in range(capacity):
                            fetch(source, k, c, True)
                    else:

                        @pl.when(code_ref[source] == code)
                        def _(source=source, k=k):
                            for c in range(capacity):
                                fetch(source, k, c, False)

        pltpu.make_async_copy(table.at[row], table.at[row], sem.at[row]).wait()
        rows_ref[0] = table[row]
        part = jnp.zeros(part_ref.shape[1:], jnp.float32)
        for s in range(kslots):
            omega = omega_ref[0, s].astype(jnp.bfloat16)
            if s > 0:
                late = late_ref[row * kslots + s]

                @pl.when(late >= 0)
                def _(late=late, omega=omega):
                    omega_late[late] = omega

                omega = jnp.where(late >= 0, jnp.zeros_like(omega), omega)
            part += jnp.dot(
                omega,
                table[row, s * block_width : (s + 1) * block_width],
                preferred_element_type=jnp.float32,
            )
        part_ref[0] = part

    return body


def gather_early(
    entries, panel_ids, codes, late, omega_blocks, own, arrays, layout, capacity, late_count
):
    row_count, kslots, block_width, _ = omega_blocks.shape
    samples = own.shape[2]
    flops = 2 * row_count * kslots * block_width * block_width * samples
    return pl.pallas_call(
        gather_kernel(layout, kslots, capacity),
        out_shape=[
            jax.ShapeDtypeStruct((row_count, block_width, samples), jnp.float32),
            jax.ShapeDtypeStruct((row_count, kslots * block_width, samples), jnp.bfloat16),
            jax.ShapeDtypeStruct((late_count, block_width, block_width), jnp.bfloat16),
        ],
        grid_spec=pltpu.PrefetchScalarGridSpec(
            num_scalar_prefetch=4,
            grid=(row_count,),
            in_specs=[pl.BlockSpec((1, kslots, block_width, block_width), lambda i, *_: (i, 0, 0, 0))]
            + [pl.BlockSpec(memory_space=pl.ANY)] * (1 + len(arrays)),
            out_specs=[
                pl.BlockSpec((1, block_width, samples), lambda i, *_: (i, 0, 0)),
                pl.BlockSpec((1, kslots * block_width, samples), lambda i, *_: (i, 0, 0)),
                pl.BlockSpec((late_count, block_width, block_width), lambda i, *_: (0, 0, 0)),
            ],
            scratch_shapes=[
                pltpu.VMEM((row_count, kslots * block_width, samples), jnp.bfloat16),
                pltpu.SemaphoreType.DMA((row_count,)),
            ],
        ),
        compiler_params=pltpu.CompilerParams(
            dimension_semantics=("arbitrary",), vmem_limit_bytes=56 << 20
        ),
        cost_estimate=pl.CostEstimate(
            flops=flops,
            transcendentals=0,
            bytes_accessed=2 * kslots * row_count * block_width * samples * 2,
        ),
        name="gather_early",
    )(entries, panel_ids, codes, late, omega_blocks, own, *arrays)


def gram_kernel(line_count, kslots, capacity, half_rows):
    def body(panel_ref, code_ref, late_ref, omega_ref, part_ref, rows_ref, *refs):
        lines = refs[:line_count]
        came = refs[line_count:-7]
        grams_ref, send_ref, table, held, w_row, sem, held_sem = refs[-7:]
        row = pl.program_id(0)
        block_width = w_row.shape[0]

        slots = table.shape[0]
        slot = row % slots

        def start(i):
            pltpu.make_async_copy(rows_ref.at[i], table.at[i % slots], sem.at[i % slots]).start()

        @pl.when(row == 0)
        def _():
            for mask, block in enumerate(came):
                at = pl.ds((mask + 1) * capacity, capacity)
                pltpu.make_async_copy(block, held.at[at], held_sem.at[0]).start()
            for k in range(line_count):

                @pl.when(code_ref[0] == k)
                def _(k=k):
                    for c in range(capacity):
                        pltpu.make_async_copy(
                            lines[k].at[panel_ref[c]], held.at[c], held_sem.at[0]
                        ).start()

            for i in range(slots - 1):
                start(i)
            pltpu.make_async_copy(held, held, held_sem.at[0]).wait()

        @pl.when(row + slots - 1 < pl.num_programs(0))
        def _():
            start(row + slots - 1)

        w_row[...] = part_ref[0]
        pltpu.make_async_copy(table.at[slot], table.at[slot], sem.at[slot]).wait()
        for s in range(1, kslots):
            late = late_ref[row * kslots + s]

            @pl.when(late >= 0)
            def _(s=s, late=late):
                panel = held[late]
                table[slot, s * block_width : (s + 1) * block_width] = panel
                w_row[...] += jnp.dot(omega_ref[late], panel, preferred_element_type=jnp.float32)

        flipped = lax.dot_general(
            table[slot],
            w_row[...].astype(jnp.bfloat16),
            (((1,), (1,)), ((), ())),
            preferred_element_type=jnp.float32,
        )
        first = code_ref[1] == 0
        for s in range(kslots):
            block = flipped[s * block_width : (s + 1) * block_width]
            grams_ref[0, s] = block
            send_ref[0, s] = jnp.where(first, block[half_rows:], block[:half_rows]).astype(
                jnp.bfloat16
            )

    return body


def grams_of(panel_ids, codes, late, omega_late, part, rows, lines, came, capacity, half_rows):
    row_count, block_width, samples = part.shape
    kslots = rows.shape[1] // block_width
    slots = min(4, row_count)
    whole = (row_count, kslots, block_width, block_width)
    flops = 2 * row_count * kslots * block_width * block_width * samples
    return pl.pallas_call(
        gram_kernel(len(lines), kslots, capacity, half_rows),
        out_shape=[
            jax.ShapeDtypeStruct(whole, jnp.float32),
            jax.ShapeDtypeStruct((row_count, kslots, half_rows, block_width), jnp.bfloat16),
        ],
        grid_spec=pltpu.PrefetchScalarGridSpec(
            num_scalar_prefetch=3,
            grid=(row_count,),
            in_specs=[
                pl.BlockSpec(omega_late.shape, lambda i, *_: (0, 0, 0)),
                pl.BlockSpec((1, block_width, samples), lambda i, *_: (i, 0, 0)),
            ]
            + [pl.BlockSpec(memory_space=pl.ANY)] * (1 + len(lines) + len(came)),
            out_specs=[
                pl.BlockSpec((1, kslots, block_width, block_width), lambda i, *_: (i, 0, 0, 0)),
                pl.BlockSpec((1, kslots, half_rows, block_width), lambda i, *_: (i, 0, 0, 0)),
            ],
            scratch_shapes=[
                pltpu.VMEM((slots, kslots * block_width, samples), jnp.bfloat16),
                pltpu.VMEM(((1 + len(came)) * capacity, block_width, samples), jnp.bfloat16),
                pltpu.VMEM((block_width, samples), jnp.float32),
                pltpu.SemaphoreType.DMA((slots,)),
                pltpu.SemaphoreType.DMA((1,)),
            ],
        ),
        compiler_params=pltpu.CompilerParams(
            dimension_semantics=("arbitrary",), vmem_limit_bytes=56 << 20
        ),
        cost_estimate=pl.CostEstimate(
            flops=flops,
            transcendentals=0,
            bytes_accessed=(kslots + 4) * row_count * block_width * samples * 2,
        ),
        name="grams",
    )(panel_ids, codes, late, omega_late, part, rows, *lines, *came)


def turn_kernel(part_ref, grams_ref, keep_ref, send_ref):
    first = part_ref[0] == 0
    half_rows = keep_ref.shape[2]
    for s in range(keep_ref.shape[1]):
        turned = grams_ref[0, s].T
        low, high = turned[:half_rows], turned[half_rows:]
        keep_ref[0, s] = jnp.where(first, low, high)
        send_ref[0, s] = jnp.where(first, high, low).astype(jnp.bfloat16)


def turned_halves(sample_part, grams, half_rows):
    row_count, kslots, block_width, _ = grams.shape
    spec = pl.BlockSpec((1, kslots, half_rows, block_width), lambda i, *_: (i, 0, 0, 0))
    shape = (row_count, kslots, half_rows, block_width)
    return pl.pallas_call(
        turn_kernel,
        out_shape=[jax.ShapeDtypeStruct(shape, jnp.float32), jax.ShapeDtypeStruct(shape, jnp.bfloat16)],
        grid_spec=pltpu.PrefetchScalarGridSpec(
            num_scalar_prefetch=1,
            grid=(row_count,),
            in_specs=[pl.BlockSpec((1,) + grams.shape[1:], lambda i, *_: (i, 0, 0, 0))],
            out_specs=[spec, spec],
        ),
        compiler_params=pltpu.CompilerParams(dimension_semantics=("arbitrary",)),
        name="turn",
    )(sample_part.reshape(1), grams)


def rows_per_step(row_count):
    return 4 if row_count % 4 == 0 else 1


def outgoing_kernel(slot_ref, half_ref, keep_ref, came_ref, own_ref, out_ref):
    rows, kslots = keep_ref.shape[:2]
    first = pl.program_id(0) * rows
    for r in range(rows):
        own_ref[r] = keep_ref[r, 0] + came_ref[r, 0].astype(jnp.float32)
        for s in range(1, kslots):
            summed = keep_ref[r, s] + came_ref[r, s].astype(jnp.float32)
            out_ref[slot_ref[(first + r) * kslots + s]] = summed.astype(jnp.bfloat16)


def outgoing_blocks(slots, sample_part, grams, came_col, slot_count):
    row_count, kslots, half_rows, block_width = came_col.shape
    rows = rows_per_step(row_count)
    spec = pl.BlockSpec((rows, kslots, half_rows, block_width), lambda i, *_: (i, 0, 0, 0))
    return pl.pallas_call(
        outgoing_kernel,
        out_shape=[
            jax.ShapeDtypeStruct((row_count, half_rows, block_width), jnp.float32),
            jax.ShapeDtypeStruct((slot_count, half_rows, block_width), jnp.bfloat16),
        ],
        grid_spec=pltpu.PrefetchScalarGridSpec(
            num_scalar_prefetch=2,
            grid=(row_count // rows,),
            in_specs=[
                pl.BlockSpec(
                    (rows, kslots, half_rows, block_width),
                    lambda i, slot, half: (i, 0, half[0], 0),
                ),
                spec,
            ],
            out_specs=[
                pl.BlockSpec((rows, half_rows, block_width), lambda i, *_: (i, 0, 0)),
                pl.BlockSpec((slot_count, half_rows, block_width), lambda i, *_: (0, 0, 0)),
            ],
        ),
        compiler_params=pltpu.CompilerParams(dimension_semantics=("arbitrary",)),
        name="outgoing",
    )(slots, sample_part.reshape(1), grams, came_col)


def final_kernel(scale):
    def body(slot_ref, half_ref, keep_ref, came_ref, own_ref, mirror_ref, omega_ref, grad_ref, next_ref):
        rows, kslots, half_rows, block_width = keep_ref.shape
        first = pl.program_id(0) * rows
        start = half_ref[0] * half_rows
        row_ids = lax.broadcasted_iota(jnp.int32, (half_rows, block_width), 0) + start
        col_ids = lax.broadcasted_iota(jnp.int32, (half_rows, block_width), 1)
        on_diagonal = row_ids == col_ids
        for r in range(rows):
            for s in range(kslots):
                omega = omega_ref[r, s]
                if s == 0:
                    mirror = own_ref[r]
                else:
                    mirror = mirror_ref[slot_ref[(first + r) * kslots + s]].astype(jnp.float32)
                gradient = (keep_ref[r, s] + came_ref[r, s].astype(jnp.float32) + mirror) * scale
                if s == 0:
                    inverse = 1.0 / jnp.where(on_diagonal, omega, 1.0)
                    gradient = gradient - jnp.where(on_diagonal, inverse, 0.0)
                trial = omega - STEP * gradient
                size = jnp.maximum(jnp.abs(trial) - STEP * PENALTY, 0.0)
                shrunk = jnp.where(trial < 0.0, -size, size)
                if s == 0:
                    shrunk = jnp.where(on_diagonal, trial, shrunk)
                grad_ref[r, s] = gradient
                next_ref[r, s] = shrunk

    return body


def final_step(slots, sample_part, keep_row, came_row, own_col, incoming, omega_blocks, scale):
    row_count, kslots, half_rows, block_width = keep_row.shape
    rows = rows_per_step(row_count)
    spec = pl.BlockSpec((rows, kslots, half_rows, block_width), lambda i, *_: (i, 0, 0, 0))
    shape = jax.ShapeDtypeStruct(keep_row.shape, jnp.float32)
    return pl.pallas_call(
        final_kernel(scale),
        out_shape=[shape, shape],
        grid_spec=pltpu.PrefetchScalarGridSpec(
            num_scalar_prefetch=2,
            grid=(row_count // rows,),
            in_specs=[
                spec,
                spec,
                pl.BlockSpec((rows, half_rows, block_width), lambda i, *_: (i, 0, 0)),
                pl.BlockSpec(incoming.shape, lambda i, *_: (0, 0, 0)),
                pl.BlockSpec(
                    (rows, kslots, half_rows, block_width),
                    lambda i, slot, half: (i, 0, half[0], 0),
                ),
            ],
            out_specs=[spec, spec],
        ),
        compiler_params=pltpu.CompilerParams(dimension_semantics=("arbitrary",)),
        name="final_step",
    )(slots, sample_part.reshape(1), keep_row, came_row, own_col, incoming, omega_blocks)


def ranks_among(same, keys):
    return jnp.sum((same & (keys[..., None, :] < keys[..., :, None])).astype(jnp.int32), axis=-1)


def step_on_device(voxel_data, omega_blocks, block_cols):
    row_count, kslots, block_width, _ = omega_blocks.shape
    devices = lax.axis_size("vars")
    samp_count = lax.axis_size("samp")
    me = lax.axis_index("vars")
    sample_part = lax.axis_index("samp")
    half_rows = block_width // samp_count
    samples = voxel_data.shape[1]
    total_samples = samples * samp_count
    capacity = 2 * ((row_count // 2 * (kslots - 1) + devices - 2) // (devices - 1))
    entries = row_count * kslots
    length = line_length(devices)
    plane = devices // length
    place, seat = me // plane, me % plane
    panels = voxel_data.reshape(row_count, block_width, samples)

    def along(array, step):
        pairs = [
            (p * plane + b, (p + step) * plane + b)
            for p in range(length)
            if 0 <= p + step < length
            for b in range(plane)
        ]
        return lax.ppermute(array, "vars", pairs)

    def across(array, mask):
        pairs = [(p * plane + b, p * plane + (b ^ mask)) for p in range(length) for b in range(plane)]
        return lax.ppermute(array, "vars", pairs)

    order = [[p] + arrivals(p, length) for p in range(length)]
    offsets = [[order[p][m] - p for p in range(length)] for m in range(length)]
    choices = [sorted(set(offsets[m])) for m in range(length)]
    sources = jnp.array(order, jnp.int32)[place]
    facts = [
        [p, b] + [choices[m].index(offsets[m][p]) for m in range(length)]
        for p in range(length)
        for b in range(plane)
    ]
    info = lax.dynamic_slice_in_dim(jnp.array(facts, jnp.int32), me, 1, 0)[0]

    came_cols = {0: block_cols}
    for m in range(1, length):
        for step in (-1, 1):
            came_cols[step * m] = along(came_cols[step * (m - 1)], -step)

    entry_ids = jnp.arange(entries, dtype=jnp.int32)
    remote = entry_ids % kslots != 0

    flat_cols = block_cols.reshape(entries)
    owners = flat_cols // row_count
    same_peer = (owners[:, None] == owners[None, :]) & remote[:, None] & remote[None, :]
    sort_keys = flat_cols * kslots + entry_ids % kslots
    entry_rank = ranks_among(same_peer, entry_ids)
    key_rank = ranks_among(same_peer, sort_keys)
    mirror_in = owners * capacity + entry_rank
    mirror_out = owners * capacity + key_rank
    peers = (
        sources[:, None] * plane + (seat ^ jnp.arange(plane, dtype=jnp.int32))[None, :]
    ).reshape(-1)
    wanted = (
        remote
        & (owners == peers[:, None])[:, None, :]
        & (key_rank == jnp.arange(capacity, dtype=jnp.int32)[:, None])[None]
    )
    entry_table = (jnp.sum(jnp.where(wanted, entry_ids + 1, 0), axis=-1) - 1).reshape(-1)
    panel_table = jnp.sum(jnp.where(wanted, flat_cols % row_count, 0), axis=-1).reshape(-1)

    late_hit = remote & (owners // plane == sources[-1])
    late = jnp.where(late_hit, ((owners % plane) ^ seat) * capacity + key_rank, -1)

    came = {0: panels}
    received = []
    for m in range(length):
        if m > 0:
            for step in (-1, 1):
                came[step * m] = along(came[step * (m - 1)], -step)
        sent = select_panels(
            m,
            info,
            [came_cols[o] for o in choices[m]],
            [came[o] for o in choices[m]],
            plane - 1,
            capacity,
        )
        received.append([across(block, mask + 1) for mask, block in enumerate(sent)])

    last = length - 1
    arrays, layout, line_users = [], [], {}
    code_values = [jnp.int32(0)] * (last * plane)
    for m in range(last):
        for mask in range(1, plane):
            arrays.append(received[m][mask - 1])
            layout.append([(m * plane + mask, None)])
        if m > 0:
            code_values[m * plane] = info[2 + m]
            for number, option in enumerate(choices[m]):
                line_users.setdefault(option, []).append((m * plane, number))
    for option in sorted(line_users):
        arrays.append(came[option])
        layout.append(line_users[option])
    early = last * plane * capacity
    part, rows, omega_late = gather_early(
        entry_table[:early],
        panel_table[:early],
        jnp.stack(code_values),
        late,
        omega_blocks,
        panels,
        arrays,
        layout,
        capacity,
        plane * capacity,
    )
    grams, send_col = grams_of(
        panel_table[early : early + capacity],
        jnp.stack([info[2 + last], sample_part]),
        late,
        omega_late,
        part,
        rows,
        [came[o] for o in choices[last]],
        received[last],
        capacity,
        half_rows,
    )

    swap = [(k, samp_count - 1 - k) for k in range(samp_count)]
    came_col = lax.ppermute(send_col, "samp", swap)
    own_col, outgoing = outgoing_blocks(
        mirror_out, sample_part, grams, came_col, devices * capacity
    )
    outgoing, grams = lax.optimization_barrier((outgoing, grams))
    incoming = lax.all_to_all(
        outgoing.reshape(devices, capacity, half_rows, block_width),
        "vars",
        split_axis=0,
        concat_axis=0,
        tiled=True,
    ).reshape(devices * capacity, half_rows, block_width)
    keep_row, send_row = turned_halves(sample_part, grams, half_rows)
    came_row = lax.ppermute(send_row, "samp", swap)
    return tuple(
        final_step(
            mirror_in,
            sample_part,
            keep_row,
            came_row,
            own_col,
            incoming,
            omega_blocks,
            0.5 / total_samples,
        )
    )


def solution(mesh):
    in_specs = (P("vars", "samp"), P("vars", None, None, None), P("vars", None))
    out_specs = (P("vars", None, "samp", None), P("vars", None, "samp", None))
    return jax.shard_map(
        step_on_device, mesh=mesh, in_specs=in_specs, out_specs=out_specs, check_vma=False
    )
```

```python
import jax
import jax.numpy as jnp
from jax import lax
from jax.experimental import pallas as pl
from jax.experimental.pallas import tpu as pltpu
from jax.sharding import PartitionSpec as P


STEP = 0.5
PENALTY = 0.1


def line_length(devices):
    bits = devices.bit_length() - 1
    return 1 << -(-bits // 3)


def arrivals(place, length):
    others = [p for p in range(length) if p != place]
    outward = 1 if 2 * place < length else -1
    return sorted(others, key=lambda p: (abs(p - place), outward * (p - place)))


def select_kernel(phase, sources, targets, capacity):
    def body(info_ref, *refs):
        cols, ins = refs[:sources], refs[sources : 2 * sources]
        outs = refs[2 * sources : 2 * sources + targets]
        held, counts, came, left = refs[2 * sources + targets :]
        row_count, kslots = cols[0].shape
        plane = targets + 1
        place, seat = info_ref[0], info_ref[1]
        for t in range(plane):
            counts[t] = 0

        for k in range(sources):

            @pl.when(info_ref[2 + phase] == k)
            def _(k=k):
                def row_step(i, carry):
                    for s in range(1, kslots):
                        owner = cols[k][i, s] // row_count
                        mask = (owner % plane) ^ seat

                        @pl.when((owner // plane == place) & (mask > 0))
                        def _():
                            c = counts[mask]
                            counts[mask] = c + 1
                            pltpu.make_async_copy(
                                ins[k].at[i], held.at[mask - 1, c], came.at[mask - 1]
                            ).start()

                    return carry

                lax.fori_loop(0, row_count, row_step, 0)

        for t in range(targets):

            def fill(c, carry, t=t):
                pltpu.make_async_copy(ins[0].at[0], held.at[t, c], came.at[t]).start()
                return carry

            lax.fori_loop(counts[t + 1], capacity, fill, 0)
        for t in range(targets):
            pltpu.make_async_copy(held.at[t], held.at[t], came.at[t]).wait()
            pltpu.make_async_copy(held.at[t], outs[t], left.at[t]).start()
        for t in range(targets):
            pltpu.make_async_copy(held.at[t], outs[t], left.at[t]).wait()

    return body


def select_panels(phase, info, cols, arrays, targets, capacity):
    _, block_width, samples = arrays[0].shape
    shape = jax.ShapeDtypeStruct((capacity, block_width, samples), arrays[0].dtype)
    moved = 2 * targets * capacity * block_width * samples * 2
    return pl.pallas_call(
        select_kernel(phase, len(arrays), targets, capacity),
        out_shape=[shape] * targets,
        in_specs=[pl.BlockSpec(memory_space=pltpu.SMEM)] * (1 + len(cols))
        + [pl.BlockSpec(memory_space=pl.ANY)] * len(arrays),
        out_specs=[pl.BlockSpec(memory_space=pl.ANY)] * targets,
        scratch_shapes=[
            pltpu.VMEM((targets, capacity, block_width, samples), arrays[0].dtype),
            pltpu.SMEM((targets + 1,), jnp.int32),
            pltpu.SemaphoreType.DMA((targets,)),
            pltpu.SemaphoreType.DMA((targets,)),
        ],
        cost_estimate=pl.CostEstimate(flops=0, transcendentals=0, bytes_accessed=moved),
        name="select_panels",
    )(info, *cols, *arrays)


def gather_kernel(layout, kslots, capacity):
    def body(entry_ref, panel_ref, code_ref, late_ref, omega_ref, own_ref, *refs):
        arrays = refs[: len(layout)]
        part_ref, table, omega_late, sem = refs[len(layout) :]
        row = pl.program_id(0)
        block_width = table.shape[1] // kslots

        def place(panel, i, s):
            at = pl.multiple_of(s * block_width, block_width)
            pltpu.make_async_copy(panel, table.at[i, pl.ds(at, block_width)], sem.at[i]).start()

        def fetch(source, k, c, fixed):
            entry = entry_ref[source * capacity + c]
            panel = c if fixed else panel_ref[source * capacity + c]

            @pl.when(entry >= 0)
            def _():
                place(arrays[k].at[panel], entry // kslots, entry % kslots)

        @pl.when(row == 0)
        def _():
            for i in range(table.shape[0]):
                place(own_ref.at[i], i, 0)
            for i in range(table.shape[0]):
                for s in range(1, kslots):

                    @pl.when(late_ref[i * kslots + s] >= 0)
                    def _(i=i, s=s):
                        place(own_ref.at[i], i, s)

            for k, users in enumerate(layout):
                for source, code in users:
                    if code is None:
                        for c in range(capacity):
                            fetch(source, k, c, True)
                    else:

                        @pl.when(code_ref[source] == code)
                        def _(source=source, k=k):
                            for c in range(capacity):
                                fetch(source, k, c, False)

        pltpu.make_async_copy(table.at[row], table.at[row], sem.at[row]).wait()
        part = jnp.zeros(part_ref.shape[1:], jnp.float32)
        for s in range(kslots):
            omega = omega_ref[0, s].astype(jnp.bfloat16)
            if s > 0:
                late = late_ref[row * kslots + s]

                @pl.when(late >= 0)
                def _(late=late, omega=omega):
                    omega_late[late] = omega

                omega = jnp.where(late >= 0, jnp.zeros_like(omega), omega)
            part += jnp.dot(
                omega,
                table[row, s * block_width : (s + 1) * block_width],
                preferred_element_type=jnp.float32,
            )
        part_ref[0] = part

    return body


def gather_early(
    entries, panel_ids, codes, late, omega_blocks, own, arrays, layout, capacity, late_count
):
    row_count, kslots, block_width, _ = omega_blocks.shape
    samples = own.shape[2]
    flops = 2 * row_count * kslots * block_width * block_width * samples
    return pl.pallas_call(
        gather_kernel(layout, kslots, capacity),
        out_shape=[
            jax.ShapeDtypeStruct((row_count, block_width, samples), jnp.float32),
            pltpu.VMEM((row_count, kslots * block_width, samples), jnp.bfloat16),
            jax.ShapeDtypeStruct((late_count, block_width, block_width), jnp.bfloat16),
        ],
        grid_spec=pltpu.PrefetchScalarGridSpec(
            num_scalar_prefetch=4,
            grid=(row_count,),
            in_specs=[pl.BlockSpec((1, kslots, block_width, block_width), lambda i, *_: (i, 0, 0, 0))]
            + [pl.BlockSpec(memory_space=pl.ANY)] * (1 + len(arrays)),
            out_specs=[
                pl.BlockSpec((1, block_width, samples), lambda i, *_: (i, 0, 0)),
                pl.BlockSpec(memory_space=pltpu.VMEM),
                pl.BlockSpec((late_count, block_width, block_width), lambda i, *_: (0, 0, 0)),
            ],
            scratch_shapes=[pltpu.SemaphoreType.DMA((row_count,))],
        ),
        compiler_params=pltpu.CompilerParams(
            dimension_semantics=("arbitrary",), vmem_limit_bytes=30 << 20
        ),
        cost_estimate=pl.CostEstimate(
            flops=flops,
            transcendentals=0,
            bytes_accessed= kslots * row_count * block_width * samples * 2,
        ),
        name="gather_early",
    )(entries, panel_ids, codes, late, omega_blocks, own, *arrays)


def gram_kernel(line_count, kslots, capacity, half_rows):
    def body(panel_ref, code_ref, late_ref, omega_ref, part_ref, rows_ref, *refs):
        lines = refs[:line_count]
        came = refs[line_count:-5]
        grams_ref, send_ref, held, w_row, held_sem = refs[-5:]
        row = pl.program_id(0)
        block_width = w_row.shape[0]

        @pl.when(row == 0)
        def _():
            for mask, block in enumerate(came):
                at = pl.ds((mask + 1) * capacity, capacity)
                pltpu.make_async_copy(block, held.at[at], held_sem.at[0]).start()
            for k in range(line_count):

                @pl.when(code_ref[0] == k)
                def _(k=k):
                    for c in range(capacity):
                        pltpu.make_async_copy(
                            lines[k].at[panel_ref[c]], held.at[c], held_sem.at[0]
                        ).start()

            pltpu.make_async_copy(held, held, held_sem.at[0]).wait()

        w_row[...] = part_ref[0]
        for s in range(1, kslots):
            late = late_ref[row * kslots + s]

            @pl.when(late >= 0)
            def _(late=late):
                w_row[...] += jnp.dot(
                    omega_ref[late], held[late], preferred_element_type=jnp.float32
                )

        w_low = w_row[...].astype(jnp.bfloat16)
        contract = (((1,), (1,)), ((), ()))
        first = code_ref[1] == 0

        def store(s, block):
            grams_ref[0, s] = block
            send_ref[0, s] = jnp.where(first, block[half_rows:], block[:half_rows]).astype(
                jnp.bfloat16
            )

        flipped = lax.dot_general(
            rows_ref[row], w_low, contract, preferred_element_type=jnp.float32
        )
        for s in range(kslots):
            store(s, flipped[s * block_width : (s + 1) * block_width])
        for s in range(1, kslots):
            late = late_ref[row * kslots + s]

            @pl.when(late >= 0)
            def _(s=s, late=late):
                block = lax.dot_general(
                    held[late],
                    w_row[...].astype(jnp.bfloat16),
                    contract,
                    preferred_element_type=jnp.float32,
                )
                store(s, block)

    return body


def grams_of(panel_ids, codes, late, omega_late, part, rows, lines, came, capacity, half_rows):
    row_count, block_width, samples = part.shape
    kslots = rows.shape[1] // block_width
    whole = (row_count, kslots, block_width, block_width)
    flops = 2 * row_count * kslots * block_width * block_width * samples
    return pl.pallas_call(
        gram_kernel(len(lines), kslots, capacity, half_rows),
        out_shape=[
            jax.ShapeDtypeStruct(whole, jnp.float32),
            jax.ShapeDtypeStruct((row_count, kslots, half_rows, block_width), jnp.bfloat16),
        ],
        grid_spec=pltpu.PrefetchScalarGridSpec(
            num_scalar_prefetch=3,
            grid=(row_count,),
            in_specs=[
                pl.BlockSpec(omega_late.shape, lambda i, *_: (0, 0, 0)),
                pl.BlockSpec((1, block_width, samples), lambda i, *_: (i, 0, 0)),
            ]
            + [pl.BlockSpec(memory_space=pltpu.VMEM)]
            + [pl.BlockSpec(memory_space=pl.ANY)] * (len(lines) + len(came)),
            out_specs=[
                pl.BlockSpec((1, kslots, block_width, block_width), lambda i, *_: (i, 0, 0, 0)),
                pl.BlockSpec((1, kslots, half_rows, block_width), lambda i, *_: (i, 0, 0, 0)),
            ],
            scratch_shapes=[
                pltpu.VMEM(((1 + len(came)) * capacity, block_width, samples), jnp.bfloat16),
                pltpu.VMEM((block_width, samples), jnp.float32),
                pltpu.SemaphoreType.DMA((1,)),
            ],
        ),
        compiler_params=pltpu.CompilerParams(
            dimension_semantics=("arbitrary",), vmem_limit_bytes=30 << 20
        ),
        cost_estimate=pl.CostEstimate(
            flops=flops,
            transcendentals=0,
            bytes_accessed=(kslots + 4) * row_count * block_width * samples * 2,
        ),
        name="grams",
    )(panel_ids, codes, late, omega_late, part, rows, *lines, *came)


def turn_kernel(part_ref, grams_ref, keep_ref, send_ref):
    first = part_ref[0] == 0
    half_rows = keep_ref.shape[2]
    for s in range(keep_ref.shape[1]):
        turned = grams_ref[0, s].T
        low, high = turned[:half_rows], turned[half_rows:]
        keep_ref[0, s] = jnp.where(first, low, high)
        send_ref[0, s] = jnp.where(first, high, low).astype(jnp.bfloat16)


def turned_halves(sample_part, grams, half_rows):
    row_count, kslots, block_width, _ = grams.shape
    spec = pl.BlockSpec((1, kslots, half_rows, block_width), lambda i, *_: (i, 0, 0, 0))
    shape = (row_count, kslots, half_rows, block_width)
    return pl.pallas_call(
        turn_kernel,
        out_shape=[jax.ShapeDtypeStruct(shape, jnp.float32), jax.ShapeDtypeStruct(shape, jnp.bfloat16)],
        grid_spec=pltpu.PrefetchScalarGridSpec(
            num_scalar_prefetch=1,
            grid=(row_count,),
            in_specs=[pl.BlockSpec((1,) + grams.shape[1:], lambda i, *_: (i, 0, 0, 0))],
            out_specs=[spec, spec],
        ),
        compiler_params=pltpu.CompilerParams(dimension_semantics=("arbitrary",)),
        name="turn",
    )(sample_part.reshape(1), grams)


def rows_per_step(row_count):
    return 4 if row_count % 4 == 0 else 1


def outgoing_kernel(slot_ref, half_ref, keep_ref, came_ref, own_ref, out_ref):
    rows, kslots = keep_ref.shape[:2]
    first = pl.program_id(0) * rows
    for r in range(rows):
        own_ref[r] = keep_ref[r, 0] + came_ref[r, 0].astype(jnp.float32)
        for s in range(1, kslots):
            summed = keep_ref[r, s] + came_ref[r, s].astype(jnp.float32)
            out_ref[slot_ref[(first + r) * kslots + s]] = summed.astype(jnp.bfloat16)


def outgoing_blocks(slots, sample_part, grams, came_col, slot_count):
    row_count, kslots, half_rows, block_width = came_col.shape
    rows = rows_per_step(row_count)
    spec = pl.BlockSpec((rows, kslots, half_rows, block_width), lambda i, *_: (i, 0, 0, 0))
    return pl.pallas_call(
        outgoing_kernel,
        out_shape=[
            jax.ShapeDtypeStruct((row_count, half_rows, block_width), jnp.float32),
            jax.ShapeDtypeStruct((slot_count, half_rows, block_width), jnp.bfloat16),
        ],
        grid_spec=pltpu.PrefetchScalarGridSpec(
            num_scalar_prefetch=2,
            grid=(row_count // rows,),
            in_specs=[
                pl.BlockSpec(
                    (rows, kslots, half_rows, block_width),
                    lambda i, slot, half: (i, 0, half[0], 0),
                ),
                spec,
            ],
            out_specs=[
                pl.BlockSpec((rows, half_rows, block_width), lambda i, *_: (i, 0, 0)),
                pl.BlockSpec((slot_count, half_rows, block_width), lambda i, *_: (0, 0, 0)),
            ],
        ),
        compiler_params=pltpu.CompilerParams(dimension_semantics=("arbitrary",)),
        name="outgoing",
    )(slots, sample_part.reshape(1), grams, came_col)


def final_kernel(scale):
    def body(slot_ref, half_ref, keep_ref, came_ref, own_ref, mirror_ref, omega_ref, grad_ref, next_ref):
        rows, kslots, half_rows, block_width = keep_ref.shape
        first = pl.program_id(0) * rows
        start = half_ref[0] * half_rows
        row_ids = lax.broadcasted_iota(jnp.int32, (half_rows, block_width), 0) + start
        col_ids = lax.broadcasted_iota(jnp.int32, (half_rows, block_width), 1)
        on_diagonal = row_ids == col_ids
        for r in range(rows):
            for s in range(kslots):
                omega = omega_ref[r, s]
                if s == 0:
                    mirror = own_ref[r]
                else:
                    mirror = mirror_ref[slot_ref[(first + r) * kslots + s]].astype(jnp.float32)
                gradient = (keep_ref[r, s] + came_ref[r, s].astype(jnp.float32) + mirror) * scale
                if s == 0:
                    inverse = 1.0 / jnp.where(on_diagonal, omega, 1.0)
                    gradient = gradient - jnp.where(on_diagonal, inverse, 0.0)
                trial = omega - STEP * gradient
                size = jnp.maximum(jnp.abs(trial) - STEP * PENALTY, 0.0)
                shrunk = jnp.where(trial < 0.0, -size, size)
                if s == 0:
                    shrunk = jnp.where(on_diagonal, trial, shrunk)
                grad_ref[r, s] = gradient
                next_ref[r, s] = shrunk

    return body


def final_step(slots, sample_part, keep_row, came_row, own_col, incoming, omega_blocks, scale):
    row_count, kslots, half_rows, block_width = keep_row.shape
    rows = rows_per_step(row_count)
    spec = pl.BlockSpec((rows, kslots, half_rows, block_width), lambda i, *_: (i, 0, 0, 0))
    shape = jax.ShapeDtypeStruct(keep_row.shape, jnp.float32)
    return pl.pallas_call(
        final_kernel(scale),
        out_shape=[shape, shape],
        grid_spec=pltpu.PrefetchScalarGridSpec(
            num_scalar_prefetch=2,
            grid=(row_count // rows,),
            in_specs=[
                spec,
                spec,
                pl.BlockSpec((rows, half_rows, block_width), lambda i, *_: (i, 0, 0)),
                pl.BlockSpec(incoming.shape, lambda i, *_: (0, 0, 0)),
                pl.BlockSpec(
                    (rows, kslots, half_rows, block_width),
                    lambda i, slot, half: (i, 0, half[0], 0),
                ),
            ],
            out_specs=[spec, spec],
        ),
        compiler_params=pltpu.CompilerParams(dimension_semantics=("arbitrary",)),
        name="final_step",
    )(slots, sample_part.reshape(1), keep_row, came_row, own_col, incoming, omega_blocks)


def ranks_among(same, keys):
    return jnp.sum((same & (keys[..., None, :] < keys[..., :, None])).astype(jnp.int32), axis=-1)


def step_on_device(voxel_data, omega_blocks, block_cols):
    row_count, kslots, block_width, _ = omega_blocks.shape
    devices = lax.axis_size("vars")
    samp_count = lax.axis_size("samp")
    me = lax.axis_index("vars")
    sample_part = lax.axis_index("samp")
    half_rows = block_width // samp_count
    samples = voxel_data.shape[1]
    total_samples = samples * samp_count
    capacity = 2 * ((row_count // 2 * (kslots - 1) + devices - 2) // (devices - 1))
    entries = row_count * kslots
    length = line_length(devices)
    plane = devices // length
    place, seat = me // plane, me % plane
    panels = voxel_data.reshape(row_count, block_width, samples)

    def along(array, step):
        pairs = [
            (p * plane + b, (p + step) * plane + b)
            for p in range(length)
            if 0 <= p + step < length
            for b in range(plane)
        ]
        return lax.ppermute(array, "vars", pairs)

    def across(array, mask):
        pairs = [(p * plane + b, p * plane + (b ^ mask)) for p in range(length) for b in range(plane)]
        return lax.ppermute(array, "vars", pairs)

    order = [[p] + arrivals(p, length) for p in range(length)]
    offsets = [[order[p][m] - p for p in range(length)] for m in range(length)]
    choices = [sorted(set(offsets[m])) for m in range(length)]
    sources = jnp.array(order, jnp.int32)[place]
    facts = [
        [p, b] + [choices[m].index(offsets[m][p]) for m in range(length)]
        for p in range(length)
        for b in range(plane)
    ]
    info = lax.dynamic_slice_in_dim(jnp.array(facts, jnp.int32), me, 1, 0)[0]

    came_cols = {0: block_cols}
    for m in range(1, length):
        for step in (-1, 1):
            came_cols[step * m] = along(block_cols, -step * m)

    entry_ids = jnp.arange(entries, dtype=jnp.int32)
    remote = entry_ids % kslots != 0

    flat_cols = block_cols.reshape(entries)
    owners = flat_cols // row_count
    same_peer = (owners[:, None] == owners[None, :]) & remote[:, None] & remote[None, :]
    sort_keys = flat_cols * kslots + entry_ids % kslots
    entry_rank = ranks_among(same_peer, entry_ids)
    key_rank = ranks_among(same_peer, sort_keys)
    mirror_in = owners * capacity + entry_rank
    mirror_out = owners * capacity + key_rank
    peers = (
        sources[:, None] * plane + (seat ^ jnp.arange(plane, dtype=jnp.int32))[None, :]
    ).reshape(-1)
    wanted = (
        remote
        & (owners == peers[:, None])[:, None, :]
        & (key_rank == jnp.arange(capacity, dtype=jnp.int32)[:, None])[None]
    )
    entry_table = (jnp.sum(jnp.where(wanted, entry_ids + 1, 0), axis=-1) - 1).reshape(-1)
    panel_table = jnp.sum(jnp.where(wanted, flat_cols % row_count, 0), axis=-1).reshape(-1)

    late_hit = remote & (owners // plane == sources[-1])
    late = jnp.where(late_hit, ((owners % plane) ^ seat) * capacity + key_rank, -1)

    came = {0: panels}
    received = []
    for m in range(length):
        if m > 0:
            for step in (-1, 1):
                came[step * m] = along(came[step * (m - 1)], -step)
        sent = select_panels(
            m,
            info,
            [came_cols[o] for o in choices[m]],
            [came[o] for o in choices[m]],
            plane - 1,
            capacity,
        )
        received.append([across(block, mask + 1) for mask, block in enumerate(sent)])

    last = length - 1
    arrays, layout, line_users = [], [], {}
    code_values = [jnp.int32(0)] * (last * plane)
    for m in range(last):
        for mask in range(1, plane):
            arrays.append(received[m][mask - 1])
            layout.append([(m * plane + mask, None)])
        if m > 0:
            code_values[m * plane] = info[2 + m]
            for number, option in enumerate(choices[m]):
                line_users.setdefault(option, []).append((m * plane, number))
    for option in sorted(line_users):
        arrays.append(came[option])
        layout.append(line_users[option])
    early = last * plane * capacity
    part, rows, omega_late = gather_early(
        entry_table[:early],
        panel_table[:early],
        jnp.stack(code_values),
        late,
        omega_blocks,
        panels,
        arrays,
        layout,
        capacity,
        plane * capacity,
    )
    rows = pltpu.with_memory_space_constraint(rows, pltpu.VMEM)
    grams, send_col = grams_of(
        panel_table[early : early + capacity],
        jnp.stack([info[2 + last], sample_part]),
        late,
        omega_late,
        part,
        rows,
        [came[o] for o in choices[last]],
        received[last],
        capacity,
        half_rows,
    )

    swap = [(k, samp_count - 1 - k) for k in range(samp_count)]
    came_col = lax.ppermute(send_col, "samp", swap)
    own_col, outgoing = outgoing_blocks(
        mirror_out, sample_part, grams, came_col, devices * capacity
    )
    outgoing, grams = lax.optimization_barrier((outgoing, grams))
    incoming = lax.all_to_all(
        outgoing.reshape(devices, capacity, half_rows, block_width),
        "vars",
        split_axis=0,
        concat_axis=0,
        tiled=True,
    ).reshape(devices * capacity, half_rows, block_width)
    keep_row, send_row = turned_halves(sample_part, grams, half_rows)
    came_row = lax.ppermute(send_row, "samp", swap)
    return tuple(
        final_step(
            mirror_in,
            sample_part,
            keep_row,
            came_row,
            own_col,
            incoming,
            omega_blocks,
            0.5 / total_samples,
        )
    )


def solution(mesh):
    in_specs = (P("vars", "samp"), P("vars", None, None, None), P("vars", None))
    out_specs = (P("vars", None, "samp", None), P("vars", None, "samp", None))
    return jax.shard_map(
        step_on_device, mesh=mesh, in_specs=in_specs, out_specs=out_specs, check_vma=False
    )
```

```python
import jax
import jax.numpy as jnp
from jax import lax
from jax.experimental import pallas as pl
from jax.experimental.pallas import tpu as pltpu
from jax.sharding import PartitionSpec as P


STEP = 0.5
PENALTY = 0.1


def line_length(devices):
    bits = devices.bit_length() - 1
    return 1 << -(-bits // 3)


def arrivals(place, length):
    others = [p for p in range(length) if p != place]
    outward = 1 if 2 * place < length else -1
    return sorted(others, key=lambda p: (abs(p - place), outward * (p - place)))


def select_kernel(phase, sources, targets, capacity):
    def body(info_ref, *refs):
        cols, ins = refs[:sources], refs[sources : 2 * sources]
        outs = refs[2 * sources : 2 * sources + targets]
        held, counts, came, left = refs[2 * sources + targets :]
        row_count, kslots = cols[0].shape
        plane = targets + 1
        place, seat = info_ref[0], info_ref[1]
        for t in range(plane):
            counts[t] = 0

        for k in range(sources):

            @pl.when(info_ref[2 + phase] == k)
            def _(k=k):
                def row_step(i, carry):
                    for s in range(1, kslots):
                        owner = cols[k][i, s] // row_count
                        mask = (owner % plane) ^ seat

                        @pl.when((owner // plane == place) & (mask > 0))
                        def _():
                            c = counts[mask]
                            counts[mask] = c + 1
                            pltpu.make_async_copy(
                                ins[k].at[i], held.at[mask - 1, c], came.at[mask - 1]
                            ).start()

                    return carry

                lax.fori_loop(0, row_count, row_step, 0)

        for t in range(targets):

            def fill(c, carry, t=t):
                pltpu.make_async_copy(ins[0].at[0], held.at[t, c], came.at[t]).start()
                return carry

            lax.fori_loop(counts[t + 1], capacity, fill, 0)
        for t in range(targets):
            pltpu.make_async_copy(held.at[t], held.at[t], came.at[t]).wait()
            pltpu.make_async_copy(held.at[t], outs[t], left.at[t]).start()
        for t in range(targets):
            pltpu.make_async_copy(held.at[t], outs[t], left.at[t]).wait()

    return body


def select_panels(phase, info, cols, arrays, targets, capacity):
    _, block_width, samples = arrays[0].shape
    shape = jax.ShapeDtypeStruct((capacity, block_width, samples), arrays[0].dtype)
    moved = 2 * targets * capacity * block_width * samples * 2
    return pl.pallas_call(
        select_kernel(phase, len(arrays), targets, capacity),
        out_shape=[shape] * targets,
        in_specs=[pl.BlockSpec(memory_space=pltpu.SMEM)] * (1 + len(cols))
        + [pl.BlockSpec(memory_space=pl.ANY)] * len(arrays),
        out_specs=[pl.BlockSpec(memory_space=pl.ANY)] * targets,
        scratch_shapes=[
            pltpu.VMEM((targets, capacity, block_width, samples), arrays[0].dtype),
            pltpu.SMEM((targets + 1,), jnp.int32),
            pltpu.SemaphoreType.DMA((targets,)),
            pltpu.SemaphoreType.DMA((targets,)),
        ],
        cost_estimate=pl.CostEstimate(flops=0, transcendentals=0, bytes_accessed=moved),
        name="select_panels",
    )(info, *cols, *arrays)


def gather_kernel(layout, kslots, capacity):
    def body(entry_ref, panel_ref, code_ref, late_ref, omega_ref, own_ref, *refs):
        arrays = refs[: len(layout)]
        part_ref, table, omega_late, sem = refs[len(layout) :]
        row = pl.program_id(0)
        block_width = table.shape[1] // kslots

        def place(panel, i, s):
            at = pl.multiple_of(s * block_width, block_width)
            pltpu.make_async_copy(panel, table.at[i, pl.ds(at, block_width)], sem.at[i]).start()

        def fetch(source, k, c, fixed):
            entry = entry_ref[source * capacity + c]
            panel = c if fixed else panel_ref[source * capacity + c]

            @pl.when(entry >= 0)
            def _():
                place(arrays[k].at[panel], entry // kslots, entry % kslots)

        @pl.when(row == 0)
        def _():
            for i in range(table.shape[0]):
                place(own_ref.at[i], i, 0)
            for i in range(table.shape[0]):
                for s in range(1, kslots):

                    @pl.when(late_ref[i * kslots + s] >= 0)
                    def _(i=i, s=s):
                        place(own_ref.at[i], i, s)

            for k, users in enumerate(layout):
                for source, code in users:
                    if code is None:
                        for c in range(capacity):
                            fetch(source, k, c, True)
                    else:

                        @pl.when(code_ref[source] == code)
                        def _(source=source, k=k):
                            for c in range(capacity):
                                fetch(source, k, c, False)

        pltpu.make_async_copy(table.at[row], table.at[row], sem.at[row]).wait()
        part = jnp.zeros(part_ref.shape[1:], jnp.float32)
        for s in range(kslots):
            omega = omega_ref[0, s].astype(jnp.bfloat16)
            if s > 0:
                late = late_ref[row * kslots + s]

                @pl.when(late >= 0)
                def _(late=late, omega=omega):
                    omega_late[late] = omega

                omega = jnp.where(late >= 0, jnp.zeros_like(omega), omega)
            part += jnp.dot(
                omega,
                table[row, s * block_width : (s + 1) * block_width],
                preferred_element_type=jnp.float32,
            )
        part_ref[0] = part

    return body


def gather_early(
    entries, panel_ids, codes, late, omega_blocks, own, arrays, layout, capacity, late_count
):
    row_count, kslots, block_width, _ = omega_blocks.shape
    samples = own.shape[2]
    flops = 2 * row_count * kslots * block_width * block_width * samples
    return pl.pallas_call(
        gather_kernel(layout, kslots, capacity),
        out_shape=[
            jax.ShapeDtypeStruct((row_count, block_width, samples), jnp.float32),
            pltpu.VMEM((row_count, kslots * block_width, samples), jnp.bfloat16),
            jax.ShapeDtypeStruct((late_count, block_width, block_width), jnp.bfloat16),
        ],
        grid_spec=pltpu.PrefetchScalarGridSpec(
            num_scalar_prefetch=4,
            grid=(row_count,),
            in_specs=[pl.BlockSpec((1, kslots, block_width, block_width), lambda i, *_: (i, 0, 0, 0))]
            + [pl.BlockSpec(memory_space=pl.ANY)] * (1 + len(arrays)),
            out_specs=[
                pl.BlockSpec((1, block_width, samples), lambda i, *_: (i, 0, 0)),
                pl.BlockSpec(memory_space=pltpu.VMEM),
                pl.BlockSpec((late_count, block_width, block_width), lambda i, *_: (0, 0, 0)),
            ],
            scratch_shapes=[pltpu.SemaphoreType.DMA((row_count,))],
        ),
        compiler_params=pltpu.CompilerParams(
            dimension_semantics=("arbitrary",), vmem_limit_bytes=30 << 20
        ),
        cost_estimate=pl.CostEstimate(
            flops=flops,
            transcendentals=0,
            bytes_accessed= kslots * row_count * block_width * samples * 2,
        ),
        name="gather_early",
    )(entries, panel_ids, codes, late, omega_blocks, own, *arrays)


def gram_kernel(line_count, kslots, capacity, half_rows):
    def body(panel_ref, code_ref, late_ref, entry_ref, omega_ref, part_ref, rows_ref, *refs):
        lines = refs[:line_count]
        came = refs[line_count:-6]
        grams_ref, send_ref, table, spare, w_row, sem = refs[-6:]
        row = pl.program_id(0)
        block_width = w_row.shape[0]

        def place(panel, c):
            entry = entry_ref[c]

            @pl.when(entry >= 0)
            def _():
                at = pl.multiple_of((entry % kslots) * block_width, block_width)
                pltpu.make_async_copy(
                    panel, table.at[entry // kslots, pl.ds(at, block_width)], sem.at[0]
                ).start()

            @pl.when(entry < 0)
            def _():
                pltpu.make_async_copy(panel, spare.at[c], sem.at[0]).start()

        @pl.when(row == 0)
        def _():
            for mask, block in enumerate(came):
                for c in range(capacity):
                    place(block.at[c], (mask + 1) * capacity + c)
            for k in range(line_count):

                @pl.when(code_ref[0] == k)
                def _(k=k):
                    for c in range(capacity):
                        place(lines[k].at[panel_ref[c]], c)

            pltpu.make_async_copy(spare, spare, sem.at[0]).wait()

        w_row[...] = part_ref[0]
        for s in range(1, kslots):
            late = late_ref[row * kslots + s]

            @pl.when(late >= 0)
            def _(s=s, late=late):
                w_row[...] += jnp.dot(
                    omega_ref[late],
                    table[row, s * block_width : (s + 1) * block_width],
                    preferred_element_type=jnp.float32,
                )

        w_low = w_row[...].astype(jnp.bfloat16)
        contract = (((1,), (1,)), ((), ()))
        first = code_ref[1] == 0

        def store(s, block):
            grams_ref[0, s] = block
            send_ref[0, s] = jnp.where(first, block[half_rows:], block[:half_rows]).astype(
                jnp.bfloat16
            )

        flipped = lax.dot_general(
            table[row], w_low, contract, preferred_element_type=jnp.float32
        )
        for s in range(kslots):
            store(s, flipped[s * block_width : (s + 1) * block_width])

    return body


def grams_of(
    panel_ids, codes, late, entries, omega_late, part, rows, lines, came, capacity, half_rows
):
    row_count, block_width, samples = part.shape
    kslots = rows.shape[1] // block_width
    whole = (row_count, kslots, block_width, block_width)
    flops = 2 * row_count * kslots * block_width * block_width * samples
    return pl.pallas_call(
        gram_kernel(len(lines), kslots, capacity, half_rows),
        out_shape=[
            jax.ShapeDtypeStruct(whole, jnp.float32),
            jax.ShapeDtypeStruct((row_count, kslots, half_rows, block_width), jnp.bfloat16),
            pltpu.VMEM(rows.shape, rows.dtype),
        ],
        grid_spec=pltpu.PrefetchScalarGridSpec(
            num_scalar_prefetch=4,
            grid=(row_count,),
            in_specs=[
                pl.BlockSpec(omega_late.shape, lambda i, *_: (0, 0, 0)),
                pl.BlockSpec((1, block_width, samples), lambda i, *_: (i, 0, 0)),
            ]
            + [pl.BlockSpec(memory_space=pltpu.VMEM)]
            + [pl.BlockSpec(memory_space=pl.ANY)] * (len(lines) + len(came)),
            out_specs=[
                pl.BlockSpec((1, kslots, block_width, block_width), lambda i, *_: (i, 0, 0, 0)),
                pl.BlockSpec((1, kslots, half_rows, block_width), lambda i, *_: (i, 0, 0, 0)),
                pl.BlockSpec(memory_space=pltpu.VMEM),
            ],
            scratch_shapes=[
                pltpu.VMEM(((1 + len(came)) * capacity, block_width, samples), jnp.bfloat16),
                pltpu.VMEM((block_width, samples), jnp.float32),
                pltpu.SemaphoreType.DMA((1,)),
            ],
        ),
        compiler_params=pltpu.CompilerParams(
            dimension_semantics=("arbitrary",), vmem_limit_bytes=30 << 20
        ),
        cost_estimate=pl.CostEstimate(
            flops=flops,
            transcendentals=0,
            bytes_accessed=(kslots + 4) * row_count * block_width * samples * 2,
        ),
        input_output_aliases={6: 2},
        name="grams",
    )(panel_ids, codes, late, entries, omega_late, part, rows, *lines, *came)


def turn_kernel(part_ref, grams_ref, keep_ref, send_ref):
    first = part_ref[0] == 0
    half_rows = keep_ref.shape[2]
    for s in range(keep_ref.shape[1]):
        turned = grams_ref[0, s].T
        low, high = turned[:half_rows], turned[half_rows:]
        keep_ref[0, s] = jnp.where(first, low, high)
        send_ref[0, s] = jnp.where(first, high, low).astype(jnp.bfloat16)


def turned_halves(sample_part, grams, half_rows):
    row_count, kslots, block_width, _ = grams.shape
    spec = pl.BlockSpec((1, kslots, half_rows, block_width), lambda i, *_: (i, 0, 0, 0))
    shape = (row_count, kslots, half_rows, block_width)
    return pl.pallas_call(
        turn_kernel,
        out_shape=[jax.ShapeDtypeStruct(shape, jnp.float32), jax.ShapeDtypeStruct(shape, jnp.bfloat16)],
        grid_spec=pltpu.PrefetchScalarGridSpec(
            num_scalar_prefetch=1,
            grid=(row_count,),
            in_specs=[pl.BlockSpec((1,) + grams.shape[1:], lambda i, *_: (i, 0, 0, 0))],
            out_specs=[spec, spec],
        ),
        compiler_params=pltpu.CompilerParams(dimension_semantics=("arbitrary",)),
        name="turn",
    )(sample_part.reshape(1), grams)


def rows_per_step(row_count):
    return 4 if row_count % 4 == 0 else 1


def outgoing_kernel(slot_ref, half_ref, keep_ref, came_ref, own_ref, out_ref):
    rows, kslots = keep_ref.shape[:2]
    first = pl.program_id(0) * rows
    for r in range(rows):
        own_ref[r] = keep_ref[r, 0] + came_ref[r, 0].astype(jnp.float32)
        for s in range(1, kslots):
            summed = keep_ref[r, s] + came_ref[r, s].astype(jnp.float32)
            out_ref[slot_ref[(first + r) * kslots + s]] = summed.astype(jnp.bfloat16)


def outgoing_blocks(slots, sample_part, grams, came_col, slot_count):
    row_count, kslots, half_rows, block_width = came_col.shape
    rows = rows_per_step(row_count)
    spec = pl.BlockSpec((rows, kslots, half_rows, block_width), lambda i, *_: (i, 0, 0, 0))
    return pl.pallas_call(
        outgoing_kernel,
        out_shape=[
            jax.ShapeDtypeStruct((row_count, half_rows, block_width), jnp.float32),
            jax.ShapeDtypeStruct((slot_count, half_rows, block_width), jnp.bfloat16),
        ],
        grid_spec=pltpu.PrefetchScalarGridSpec(
            num_scalar_prefetch=2,
            grid=(row_count // rows,),
            in_specs=[
                pl.BlockSpec(
                    (rows, kslots, half_rows, block_width),
                    lambda i, slot, half: (i, 0, half[0], 0),
                ),
                spec,
            ],
            out_specs=[
                pl.BlockSpec((rows, half_rows, block_width), lambda i, *_: (i, 0, 0)),
                pl.BlockSpec((slot_count, half_rows, block_width), lambda i, *_: (0, 0, 0)),
            ],
        ),
        compiler_params=pltpu.CompilerParams(dimension_semantics=("arbitrary",)),
        name="outgoing",
    )(slots, sample_part.reshape(1), grams, came_col)


def final_kernel(scale):
    def body(slot_ref, half_ref, keep_ref, came_ref, own_ref, mirror_ref, omega_ref, grad_ref, next_ref):
        rows, kslots, half_rows, block_width = keep_ref.shape
        first = pl.program_id(0) * rows
        start = half_ref[0] * half_rows
        row_ids = lax.broadcasted_iota(jnp.int32, (half_rows, block_width), 0) + start
        col_ids = lax.broadcasted_iota(jnp.int32, (half_rows, block_width), 1)
        on_diagonal = row_ids == col_ids
        for r in range(rows):
            for s in range(kslots):
                omega = omega_ref[r, s]
                if s == 0:
                    mirror = own_ref[r]
                else:
                    mirror = mirror_ref[slot_ref[(first + r) * kslots + s]].astype(jnp.float32)
                gradient = (keep_ref[r, s] + came_ref[r, s].astype(jnp.float32) + mirror) * scale
                if s == 0:
                    inverse = 1.0 / jnp.where(on_diagonal, omega, 1.0)
                    gradient = gradient - jnp.where(on_diagonal, inverse, 0.0)
                trial = omega - STEP * gradient
                size = jnp.maximum(jnp.abs(trial) - STEP * PENALTY, 0.0)
                shrunk = jnp.where(trial < 0.0, -size, size)
                if s == 0:
                    shrunk = jnp.where(on_diagonal, trial, shrunk)
                grad_ref[r, s] = gradient
                next_ref[r, s] = shrunk

    return body


def final_step(slots, sample_part, keep_row, came_row, own_col, incoming, omega_blocks, scale):
    row_count, kslots, half_rows, block_width = keep_row.shape
    rows = rows_per_step(row_count)
    spec = pl.BlockSpec((rows, kslots, half_rows, block_width), lambda i, *_: (i, 0, 0, 0))
    shape = jax.ShapeDtypeStruct(keep_row.shape, jnp.float32)
    return pl.pallas_call(
        final_kernel(scale),
        out_shape=[shape, shape],
        grid_spec=pltpu.PrefetchScalarGridSpec(
            num_scalar_prefetch=2,
            grid=(row_count // rows,),
            in_specs=[
                spec,
                spec,
                pl.BlockSpec((rows, half_rows, block_width), lambda i, *_: (i, 0, 0)),
                pl.BlockSpec(incoming.shape, lambda i, *_: (0, 0, 0)),
                pl.BlockSpec(
                    (rows, kslots, half_rows, block_width),
                    lambda i, slot, half: (i, 0, half[0], 0),
                ),
            ],
            out_specs=[spec, spec],
        ),
        compiler_params=pltpu.CompilerParams(dimension_semantics=("arbitrary",)),
        name="final_step",
    )(slots, sample_part.reshape(1), keep_row, came_row, own_col, incoming, omega_blocks)


def ranks_among(same, keys):
    return jnp.sum((same & (keys[..., None, :] < keys[..., :, None])).astype(jnp.int32), axis=-1)


def step_on_device(voxel_data, omega_blocks, block_cols):
    row_count, kslots, block_width, _ = omega_blocks.shape
    devices = lax.axis_size("vars")
    samp_count = lax.axis_size("samp")
    me = lax.axis_index("vars")
    sample_part = lax.axis_index("samp")
    half_rows = block_width // samp_count
    samples = voxel_data.shape[1]
    total_samples = samples * samp_count
    capacity = 2 * ((row_count // 2 * (kslots - 1) + devices - 2) // (devices - 1))
    entries = row_count * kslots
    length = line_length(devices)
    plane = devices // length
    place, seat = me // plane, me % plane
    panels = voxel_data.reshape(row_count, block_width, samples)

    def along(array, step):
        pairs = [
            (p * plane + b, (p + step) * plane + b)
            for p in range(length)
            if 0 <= p + step < length
            for b in range(plane)
        ]
        return lax.ppermute(array, "vars", pairs)

    def across(array, mask):
        pairs = [(p * plane + b, p * plane + (b ^ mask)) for p in range(length) for b in range(plane)]
        return lax.ppermute(array, "vars", pairs)

    order = [[p] + arrivals(p, length) for p in range(length)]
    offsets = [[order[p][m] - p for p in range(length)] for m in range(length)]
    choices = [sorted(set(offsets[m])) for m in range(length)]
    sources = jnp.array(order, jnp.int32)[place]
    facts = [
        [p, b] + [choices[m].index(offsets[m][p]) for m in range(length)]
        for p in range(length)
        for b in range(plane)
    ]
    info = lax.dynamic_slice_in_dim(jnp.array(facts, jnp.int32), me, 1, 0)[0]

    came_cols = {0: block_cols}
    for m in range(1, length):
        for step in (-1, 1):
            came_cols[step * m] = along(block_cols, -step * m)

    entry_ids = jnp.arange(entries, dtype=jnp.int32)
    remote = entry_ids % kslots != 0

    flat_cols = block_cols.reshape(entries)
    owners = flat_cols // row_count
    same_peer = (owners[:, None] == owners[None, :]) & remote[:, None] & remote[None, :]
    sort_keys = flat_cols * kslots + entry_ids % kslots
    entry_rank = ranks_among(same_peer, entry_ids)
    key_rank = ranks_among(same_peer, sort_keys)
    mirror_in = owners * capacity + entry_rank
    mirror_out = owners * capacity + key_rank
    peers = (
        sources[:, None] * plane + (seat ^ jnp.arange(plane, dtype=jnp.int32))[None, :]
    ).reshape(-1)
    wanted = (
        remote
        & (owners == peers[:, None])[:, None, :]
        & (key_rank == jnp.arange(capacity, dtype=jnp.int32)[:, None])[None]
    )
    entry_table = (jnp.sum(jnp.where(wanted, entry_ids + 1, 0), axis=-1) - 1).reshape(-1)
    panel_table = jnp.sum(jnp.where(wanted, flat_cols % row_count, 0), axis=-1).reshape(-1)

    late_hit = remote & (owners // plane == sources[-1])
    late = jnp.where(late_hit, ((owners % plane) ^ seat) * capacity + key_rank, -1)

    came = {0: panels}
    received = []
    for m in range(length):
        if m > 0:
            for step in (-1, 1):
                came[step * m] = along(came[step * (m - 1)], -step)
        sent = select_panels(
            m,
            info,
            [came_cols[o] for o in choices[m]],
            [came[o] for o in choices[m]],
            plane - 1,
            capacity,
        )
        received.append([across(block, mask + 1) for mask, block in enumerate(sent)])

    last = length - 1
    arrays, layout, line_users = [], [], {}
    code_values = [jnp.int32(0)] * (last * plane)
    for m in range(last):
        for mask in range(1, plane):
            arrays.append(received[m][mask - 1])
            layout.append([(m * plane + mask, None)])
        if m > 0:
            code_values[m * plane] = info[2 + m]
            for number, option in enumerate(choices[m]):
                line_users.setdefault(option, []).append((m * plane, number))
    for option in sorted(line_users):
        arrays.append(came[option])
        layout.append(line_users[option])
    early = last * plane * capacity
    part, rows, omega_late = gather_early(
        entry_table[:early],
        panel_table[:early],
        jnp.stack(code_values),
        late,
        omega_blocks,
        panels,
        arrays,
        layout,
        capacity,
        plane * capacity,
    )
    rows = pltpu.with_memory_space_constraint(rows, pltpu.VMEM)
    grams, send_col, _ = grams_of(
        panel_table[early : early + capacity],
        jnp.stack([info[2 + last], sample_part]),
        late,
        entry_table[early:],
        omega_late,
        part,
        rows,
        [came[o] for o in choices[last]],
        received[last],
        capacity,
        half_rows,
    )

    swap = [(k, samp_count - 1 - k) for k in range(samp_count)]
    came_col = lax.ppermute(send_col, "samp", swap)
    own_col, outgoing = outgoing_blocks(
        mirror_out, sample_part, grams, came_col, devices * capacity
    )
    outgoing, grams = lax.optimization_barrier((outgoing, grams))
    incoming = lax.all_to_all(
        outgoing.reshape(devices, capacity, half_rows, block_width),
        "vars",
        split_axis=0,
        concat_axis=0,
        tiled=True,
    ).reshape(devices * capacity, half_rows, block_width)
    keep_row, send_row = turned_halves(sample_part, grams, half_rows)
    came_row = lax.ppermute(send_row, "samp", swap)
    return tuple(
        final_step(
            mirror_in,
            sample_part,
            keep_row,
            came_row,
            own_col,
            incoming,
            omega_blocks,
            0.5 / total_samples,
        )
    )


def solution(mesh):
    in_specs = (P("vars", "samp"), P("vars", None, None, None), P("vars", None))
    out_specs = (P("vars", None, "samp", None), P("vars", None, "samp", None))
    return jax.shard_map(
        step_on_device, mesh=mesh, in_specs=in_specs, out_specs=out_specs, check_vma=False
    )
```

```python
import jax
import jax.numpy as jnp
from jax import lax
from jax.experimental import pallas as pl
from jax.experimental.pallas import tpu as pltpu
from jax.sharding import PartitionSpec as P


STEP = 0.5
PENALTY = 0.1


def line_length(devices):
    bits = devices.bit_length() - 1
    return 1 << -(-bits // 3)


def arrivals(place, length):
    others = [p for p in range(length) if p != place]
    outward = 1 if 2 * place < length else -1
    return sorted(others, key=lambda p: (abs(p - place), outward * (p - place)))


def select_kernel(phase, sources, targets, capacity):
    def body(info_ref, *refs):
        cols, ins = refs[:sources], refs[sources : 2 * sources]
        outs = refs[2 * sources : 2 * sources + targets]
        held, counts, came, left = refs[2 * sources + targets :]
        row_count, kslots = cols[0].shape
        plane = targets + 1
        place, seat = info_ref[0], info_ref[1]
        for t in range(plane):
            counts[t] = 0

        for k in range(sources):

            @pl.when(info_ref[2 + phase] == k)
            def _(k=k):
                def row_step(i, carry):
                    for s in range(1, kslots):
                        owner = cols[k][i, s] // row_count
                        mask = (owner % plane) ^ seat

                        @pl.when((owner // plane == place) & (mask > 0))
                        def _():
                            c = counts[mask]
                            counts[mask] = c + 1
                            pltpu.make_async_copy(
                                ins[k].at[i], held.at[mask - 1, c], came.at[mask - 1]
                            ).start()

                    return carry

                lax.fori_loop(0, row_count, row_step, 0)

        for t in range(targets):

            def fill(c, carry, t=t):
                pltpu.make_async_copy(ins[0].at[0], held.at[t, c], came.at[t]).start()
                return carry

            lax.fori_loop(counts[t + 1], capacity, fill, 0)
        for t in range(targets):
            pltpu.make_async_copy(held.at[t], held.at[t], came.at[t]).wait()
            pltpu.make_async_copy(held.at[t], outs[t], left.at[t]).start()
        for t in range(targets):
            pltpu.make_async_copy(held.at[t], outs[t], left.at[t]).wait()

    return body


def select_panels(phase, info, cols, arrays, targets, capacity):
    _, block_width, samples = arrays[0].shape
    shape = jax.ShapeDtypeStruct((capacity, block_width, samples), arrays[0].dtype)
    moved = 2 * targets * capacity * block_width * samples * 2
    return pl.pallas_call(
        select_kernel(phase, len(arrays), targets, capacity),
        out_shape=[shape] * targets,
        in_specs=[pl.BlockSpec(memory_space=pltpu.SMEM)] * (1 + len(cols))
        + [pl.BlockSpec(memory_space=pl.ANY)] * len(arrays),
        out_specs=[pl.BlockSpec(memory_space=pl.ANY)] * targets,
        scratch_shapes=[
            pltpu.VMEM((targets, capacity, block_width, samples), arrays[0].dtype),
            pltpu.SMEM((targets + 1,), jnp.int32),
            pltpu.SemaphoreType.DMA((targets,)),
            pltpu.SemaphoreType.DMA((targets,)),
        ],
        cost_estimate=pl.CostEstimate(flops=0, transcendentals=0, bytes_accessed=moved),
        name="select_panels",
    )(info, *cols, *arrays)


def gather_kernel(layout, kslots, capacity):
    def body(entry_ref, panel_ref, code_ref, late_ref, omega_ref, own_ref, *refs):
        arrays = refs[: len(layout)]
        part_ref, table, omega_late, sem = refs[len(layout) :]
        row = pl.program_id(0)
        block_width = table.shape[1] // kslots

        def place(panel, i, s):
            at = pl.multiple_of(s * block_width, block_width)
            pltpu.make_async_copy(panel, table.at[i, pl.ds(at, block_width)], sem.at[i]).start()

        def fetch(source, k, c, fixed):
            entry = entry_ref[source * capacity + c]
            panel = c if fixed else panel_ref[source * capacity + c]

            @pl.when(entry >= 0)
            def _():
                place(arrays[k].at[panel], entry // kslots, entry % kslots)

        @pl.when(row == 0)
        def _():
            for i in range(table.shape[0]):
                place(own_ref.at[i], i, 0)
            for i in range(table.shape[0]):
                for s in range(1, kslots):

                    @pl.when(late_ref[i * kslots + s] >= 0)
                    def _(i=i, s=s):
                        place(own_ref.at[i], i, s)

            for k, users in enumerate(layout):
                for source, code in users:
                    if code is None:
                        for c in range(capacity):
                            fetch(source, k, c, True)
                    else:

                        @pl.when(code_ref[source] == code)
                        def _(source=source, k=k):
                            for c in range(capacity):
                                fetch(source, k, c, False)

        pltpu.make_async_copy(table.at[row], table.at[row], sem.at[row]).wait()
        part = jnp.zeros(part_ref.shape[1:], jnp.float32)
        for s in range(kslots):
            omega = omega_ref[0, s].astype(jnp.bfloat16)
            if s > 0:
                late = late_ref[row * kslots + s]

                @pl.when(late >= 0)
                def _(late=late, omega=omega):
                    omega_late[late] = omega

                omega = jnp.where(late >= 0, jnp.zeros_like(omega), omega)
            part += jnp.dot(
                omega,
                table[row, s * block_width : (s + 1) * block_width],
                preferred_element_type=jnp.float32,
            )
        part_ref[0] = part

    return body


def gather_early(
    entries, panel_ids, codes, late, omega_blocks, own, arrays, layout, capacity, late_count
):
    row_count, kslots, block_width, _ = omega_blocks.shape
    samples = own.shape[2]
    flops = 2 * row_count * kslots * block_width * block_width * samples
    return pl.pallas_call(
        gather_kernel(layout, kslots, capacity),
        out_shape=[
            jax.ShapeDtypeStruct((row_count, block_width, samples), jnp.float32),
            pltpu.VMEM((row_count, kslots * block_width, samples), jnp.bfloat16),
            jax.ShapeDtypeStruct((late_count, block_width, block_width), jnp.bfloat16),
        ],
        grid_spec=pltpu.PrefetchScalarGridSpec(
            num_scalar_prefetch=4,
            grid=(row_count,),
            in_specs=[pl.BlockSpec((1, kslots, block_width, block_width), lambda i, *_: (i, 0, 0, 0))]
            + [pl.BlockSpec(memory_space=pl.ANY)] * (1 + len(arrays)),
            out_specs=[
                pl.BlockSpec((1, block_width, samples), lambda i, *_: (i, 0, 0)),
                pl.BlockSpec(memory_space=pltpu.VMEM),
                pl.BlockSpec((late_count, block_width, block_width), lambda i, *_: (0, 0, 0)),
            ],
            scratch_shapes=[pltpu.SemaphoreType.DMA((row_count,))],
        ),
        compiler_params=pltpu.CompilerParams(
            dimension_semantics=("arbitrary",), vmem_limit_bytes=30 << 20
        ),
        cost_estimate=pl.CostEstimate(
            flops=flops,
            transcendentals=0,
            bytes_accessed= kslots * row_count * block_width * samples * 2,
        ),
        name="gather_early",
    )(entries, panel_ids, codes, late, omega_blocks, own, *arrays)


def gram_kernel(line_count, kslots, capacity, half_rows):
    def body(panel_ref, code_ref, late_ref, entry_ref, omega_ref, part_ref, rows_ref, *refs):
        lines = refs[:line_count]
        came = refs[line_count:-6]
        grams_ref, send_ref, table, spare, w_row, sem = refs[-6:]
        row = pl.program_id(0)
        block_width = w_row.shape[0]

        def place(panel, c):
            entry = entry_ref[c]

            @pl.when(entry >= 0)
            def _():
                at = pl.multiple_of((entry % kslots) * block_width, block_width)
                pltpu.make_async_copy(
                    panel, table.at[entry // kslots, pl.ds(at, block_width)], sem.at[0]
                ).start()

            @pl.when(entry < 0)
            def _():
                pltpu.make_async_copy(panel, spare.at[c], sem.at[0]).start()

        @pl.when(row == 0)
        def _():
            for mask, block in enumerate(came):
                for c in range(capacity):
                    place(block.at[c], (mask + 1) * capacity + c)
            for k in range(line_count):

                @pl.when(code_ref[0] == k)
                def _(k=k):
                    for c in range(capacity):
                        place(lines[k].at[panel_ref[c]], c)

            pltpu.make_async_copy(spare, spare, sem.at[0]).wait()

        w_row[...] = part_ref[0]
        for s in range(1, kslots):
            late = late_ref[row * kslots + s]

            @pl.when(late >= 0)
            def _(s=s, late=late):
                w_row[...] += jnp.dot(
                    omega_ref[late],
                    table[row, s * block_width : (s + 1) * block_width],
                    preferred_element_type=jnp.float32,
                )

        w_low = w_row[...].astype(jnp.bfloat16)
        contract = (((1,), (1,)), ((), ()))
        first = code_ref[1] == 0

        def store(s, block):
            grams_ref[0, s] = block
            send_ref[0, s] = jnp.where(first, block[half_rows:], block[:half_rows]).astype(
                jnp.bfloat16
            )

        flipped = lax.dot_general(
            table[row], w_low, contract, preferred_element_type=jnp.float32
        )
        for s in range(kslots):
            store(s, flipped[s * block_width : (s + 1) * block_width])

    return body


def grams_of(
    panel_ids, codes, late, entries, omega_late, part, rows, lines, came, capacity, half_rows
):
    row_count, block_width, samples = part.shape
    kslots = rows.shape[1] // block_width
    whole = (row_count, kslots, block_width, block_width)
    flops = 2 * row_count * kslots * block_width * block_width * samples
    return pl.pallas_call(
        gram_kernel(len(lines), kslots, capacity, half_rows),
        out_shape=[
            jax.ShapeDtypeStruct(whole, jnp.float32),
            jax.ShapeDtypeStruct((row_count, kslots, half_rows, block_width), jnp.bfloat16),
            pltpu.VMEM(rows.shape, rows.dtype),
        ],
        grid_spec=pltpu.PrefetchScalarGridSpec(
            num_scalar_prefetch=4,
            grid=(row_count,),
            in_specs=[
                pl.BlockSpec(omega_late.shape, lambda i, *_: (0, 0, 0)),
                pl.BlockSpec((1, block_width, samples), lambda i, *_: (i, 0, 0)),
            ]
            + [pl.BlockSpec(memory_space=pltpu.VMEM)]
            + [pl.BlockSpec(memory_space=pl.ANY)] * (len(lines) + len(came)),
            out_specs=[
                pl.BlockSpec((1, kslots, block_width, block_width), lambda i, *_: (i, 0, 0, 0)),
                pl.BlockSpec((1, kslots, half_rows, block_width), lambda i, *_: (i, 0, 0, 0)),
                pl.BlockSpec(memory_space=pltpu.VMEM),
            ],
            scratch_shapes=[
                pltpu.VMEM(((1 + len(came)) * capacity, block_width, samples), jnp.bfloat16),
                pltpu.VMEM((block_width, samples), jnp.float32),
                pltpu.SemaphoreType.DMA((1,)),
            ],
        ),
        compiler_params=pltpu.CompilerParams(
            dimension_semantics=("arbitrary",), vmem_limit_bytes=30 << 20
        ),
        cost_estimate=pl.CostEstimate(
            flops=flops,
            transcendentals=0,
            bytes_accessed=(kslots + 4) * row_count * block_width * samples * 2,
        ),
        input_output_aliases={6: 2},
        name="grams",
    )(panel_ids, codes, late, entries, omega_late, part, rows, *lines, *came)


def turn_kernel(part_ref, grams_ref, keep_ref, send_ref):
    first = part_ref[0] == 0
    half_rows = keep_ref.shape[2]
    for s in range(keep_ref.shape[1]):
        turned = grams_ref[0, s].T
        low, high = turned[:half_rows], turned[half_rows:]
        keep_ref[0, s] = jnp.where(first, low, high)
        send_ref[0, s] = jnp.where(first, high, low).astype(jnp.bfloat16)


def turned_halves(sample_part, grams, half_rows):
    row_count, kslots, block_width, _ = grams.shape
    spec = pl.BlockSpec((1, kslots, half_rows, block_width), lambda i, *_: (i, 0, 0, 0))
    shape = (row_count, kslots, half_rows, block_width)
    return pl.pallas_call(
        turn_kernel,
        out_shape=[jax.ShapeDtypeStruct(shape, jnp.float32), jax.ShapeDtypeStruct(shape, jnp.bfloat16)],
        grid_spec=pltpu.PrefetchScalarGridSpec(
            num_scalar_prefetch=1,
            grid=(row_count,),
            in_specs=[pl.BlockSpec((1,) + grams.shape[1:], lambda i, *_: (i, 0, 0, 0))],
            out_specs=[spec, spec],
        ),
        compiler_params=pltpu.CompilerParams(dimension_semantics=("arbitrary",)),
        name="turn",
    )(sample_part.reshape(1), grams)


def rows_per_step(row_count):
    return 4 if row_count % 4 == 0 else 1


def outgoing_kernel(slot_ref, half_ref, keep_ref, came_ref, own_ref, out_ref):
    rows, kslots = keep_ref.shape[:2]
    first = pl.program_id(0) * rows
    for r in range(rows):
        own_ref[r] = keep_ref[r, 0] + came_ref[r, 0].astype(jnp.float32)
        for s in range(1, kslots):
            summed = keep_ref[r, s] + came_ref[r, s].astype(jnp.float32)
            out_ref[slot_ref[(first + r) * kslots + s]] = summed.astype(jnp.bfloat16)


def outgoing_blocks(slots, sample_part, grams, came_col, slot_count):
    row_count, kslots, half_rows, block_width = came_col.shape
    rows = rows_per_step(row_count)
    return pl.pallas_call(
        outgoing_kernel,
        out_shape=[
            jax.ShapeDtypeStruct((row_count, half_rows, block_width), jnp.float32),
            jax.ShapeDtypeStruct((slot_count, half_rows, block_width), jnp.bfloat16),
        ],
        grid_spec=pltpu.PrefetchScalarGridSpec(
            num_scalar_prefetch=2,
            grid=(row_count // rows,),
            in_specs=[
                pl.BlockSpec(
                    (rows, kslots, half_rows, block_width),
                    lambda i, slot, half: (i, 0, half[0], 0),
                ),
                pl.BlockSpec((rows, kslots, half_rows, block_width), lambda i, *_: (i, 0, 0, 0)),
            ],
            out_specs=[
                pl.BlockSpec((rows, half_rows, block_width), lambda i, *_: (i, 0, 0)),
                pl.BlockSpec((slot_count, half_rows, block_width), lambda i, *_: (0, 0, 0)),
            ],
        ),
        compiler_params=pltpu.CompilerParams(dimension_semantics=("arbitrary",)),
        name="outgoing",
    )(slots, sample_part.reshape(1), grams, came_col)


def final_kernel(scale):
    def body(slot_ref, half_ref, keep_ref, came_ref, own_ref, mirror_ref, omega_ref, grad_ref, next_ref):
        rows, kslots, half_rows, block_width = keep_ref.shape
        first = pl.program_id(0) * rows
        start = half_ref[0] * half_rows
        row_ids = lax.broadcasted_iota(jnp.int32, (half_rows, block_width), 0) + start
        col_ids = lax.broadcasted_iota(jnp.int32, (half_rows, block_width), 1)
        on_diagonal = row_ids == col_ids
        for r in range(rows):
            for s in range(kslots):
                omega = omega_ref[r, s]
                if s == 0:
                    mirror = own_ref[r]
                else:
                    mirror = mirror_ref[slot_ref[(first + r) * kslots + s]].astype(jnp.float32)
                gradient = (keep_ref[r, s] + came_ref[r, s].astype(jnp.float32) + mirror) * scale
                if s == 0:
                    inverse = 1.0 / jnp.where(on_diagonal, omega, 1.0)
                    gradient = gradient - jnp.where(on_diagonal, inverse, 0.0)
                trial = omega - STEP * gradient
                size = jnp.maximum(jnp.abs(trial) - STEP * PENALTY, 0.0)
                shrunk = jnp.where(trial < 0.0, -size, size)
                if s == 0:
                    shrunk = jnp.where(on_diagonal, trial, shrunk)
                grad_ref[r, s] = gradient
                next_ref[r, s] = shrunk

    return body


def final_step(slots, sample_part, keep_row, came_row, own_col, incoming, omega_blocks, scale):
    row_count, kslots, half_rows, block_width = keep_row.shape
    rows = rows_per_step(row_count)
    spec = pl.BlockSpec((rows, kslots, half_rows, block_width), lambda i, *_: (i, 0, 0, 0))
    shape = jax.ShapeDtypeStruct(keep_row.shape, jnp.float32)
    return pl.pallas_call(
        final_kernel(scale),
        out_shape=[shape, shape],
        grid_spec=pltpu.PrefetchScalarGridSpec(
            num_scalar_prefetch=2,
            grid=(row_count // rows,),
            in_specs=[
                spec,
                spec,
                pl.BlockSpec((rows, half_rows, block_width), lambda i, *_: (i, 0, 0)),
                pl.BlockSpec(memory_space=pltpu.VMEM),
                pl.BlockSpec(
                    (rows, kslots, half_rows, block_width),
                    lambda i, slot, half: (i, 0, half[0], 0),
                ),
            ],
            out_specs=[spec, spec],
        ),
        compiler_params=pltpu.CompilerParams(dimension_semantics=("arbitrary",)),
        name="final_step",
    )(slots, sample_part.reshape(1), keep_row, came_row, own_col, incoming, omega_blocks)


def ranks_among(same, keys):
    return jnp.sum((same & (keys[..., None, :] < keys[..., :, None])).astype(jnp.int32), axis=-1)


def step_on_device(voxel_data, omega_blocks, block_cols):
    row_count, kslots, block_width, _ = omega_blocks.shape
    devices = lax.axis_size("vars")
    samp_count = lax.axis_size("samp")
    me = lax.axis_index("vars")
    sample_part = lax.axis_index("samp")
    half_rows = block_width // samp_count
    samples = voxel_data.shape[1]
    total_samples = samples * samp_count
    capacity = 2 * ((row_count // 2 * (kslots - 1) + devices - 2) // (devices - 1))
    entries = row_count * kslots
    length = line_length(devices)
    plane = devices // length
    place, seat = me // plane, me % plane
    panels = voxel_data.reshape(row_count, block_width, samples)

    def along(array, step):
        pairs = [
            (p * plane + b, (p + step) * plane + b)
            for p in range(length)
            if 0 <= p + step < length
            for b in range(plane)
        ]
        return lax.ppermute(array, "vars", pairs)

    def across(array, mask):
        pairs = [(p * plane + b, p * plane + (b ^ mask)) for p in range(length) for b in range(plane)]
        return lax.ppermute(array, "vars", pairs)

    order = [[p] + arrivals(p, length) for p in range(length)]
    offsets = [[order[p][m] - p for p in range(length)] for m in range(length)]
    choices = [sorted(set(offsets[m])) for m in range(length)]
    sources = jnp.array(order, jnp.int32)[place]
    facts = [
        [p, b] + [choices[m].index(offsets[m][p]) for m in range(length)]
        for p in range(length)
        for b in range(plane)
    ]
    info = lax.dynamic_slice_in_dim(jnp.array(facts, jnp.int32), me, 1, 0)[0]

    came_cols = {0: block_cols}
    for m in range(1, length):
        for step in (-1, 1):
            came_cols[step * m] = along(block_cols, -step * m)

    entry_ids = jnp.arange(entries, dtype=jnp.int32)
    remote = entry_ids % kslots != 0

    flat_cols = block_cols.reshape(entries)
    owners = flat_cols // row_count
    same_peer = (owners[:, None] == owners[None, :]) & remote[:, None] & remote[None, :]
    sort_keys = flat_cols * kslots + entry_ids % kslots
    entry_rank = ranks_among(same_peer, entry_ids)
    key_rank = ranks_among(same_peer, sort_keys)
    mirror_in = owners * capacity + entry_rank
    mirror_out = owners * capacity + key_rank
    peers = (
        sources[:, None] * plane + (seat ^ jnp.arange(plane, dtype=jnp.int32))[None, :]
    ).reshape(-1)
    wanted = (
        remote
        & (owners == peers[:, None])[:, None, :]
        & (key_rank == jnp.arange(capacity, dtype=jnp.int32)[:, None])[None]
    )
    entry_table = (jnp.sum(jnp.where(wanted, entry_ids + 1, 0), axis=-1) - 1).reshape(-1)
    panel_table = jnp.sum(jnp.where(wanted, flat_cols % row_count, 0), axis=-1).reshape(-1)

    late_hit = remote & (owners // plane == sources[-1])
    late = jnp.where(late_hit, ((owners % plane) ^ seat) * capacity + key_rank, -1)

    came = {0: panels}
    received = []
    for m in range(length):
        if m > 0:
            for step in (-1, 1):
                came[step * m] = along(came[step * (m - 1)], -step)
        sent = select_panels(
            m,
            info,
            [came_cols[o] for o in choices[m]],
            [came[o] for o in choices[m]],
            plane - 1,
            capacity,
        )
        received.append([across(block, mask + 1) for mask, block in enumerate(sent)])

    last = length - 1
    arrays, layout, line_users = [], [], {}
    code_values = [jnp.int32(0)] * (last * plane)
    for m in range(last):
        for mask in range(1, plane):
            arrays.append(received[m][mask - 1])
            layout.append([(m * plane + mask, None)])
        if m > 0:
            code_values[m * plane] = info[2 + m]
            for number, option in enumerate(choices[m]):
                line_users.setdefault(option, []).append((m * plane, number))
    for option in sorted(line_users):
        arrays.append(came[option])
        layout.append(line_users[option])
    early = last * plane * capacity
    part, rows, omega_late = gather_early(
        entry_table[:early],
        panel_table[:early],
        jnp.stack(code_values),
        late,
        omega_blocks,
        panels,
        arrays,
        layout,
        capacity,
        plane * capacity,
    )
    rows = pltpu.with_memory_space_constraint(rows, pltpu.VMEM)
    grams, send_col, _ = grams_of(
        panel_table[early : early + capacity],
        jnp.stack([info[2 + last], sample_part]),
        late,
        entry_table[early:],
        omega_late,
        part,
        rows,
        [came[o] for o in choices[last]],
        received[last],
        capacity,
        half_rows,
    )

    swap = [(k, samp_count - 1 - k) for k in range(samp_count)]
    came_col = lax.ppermute(send_col, "samp", swap)
    own_col, outgoing = outgoing_blocks(
        mirror_out, sample_part, grams, came_col, devices * capacity
    )
    outgoing, grams = lax.optimization_barrier((outgoing, grams))
    incoming = lax.all_to_all(
        outgoing.reshape(devices, capacity, half_rows, block_width),
        "vars",
        split_axis=0,
        concat_axis=0,
        tiled=True,
    ).reshape(devices * capacity, half_rows, block_width)
    incoming = pltpu.with_memory_space_constraint(incoming, pltpu.VMEM)
    keep_row, send_row = turned_halves(sample_part, grams, half_rows)
    came_row = lax.ppermute(send_row, "samp", swap)
    return tuple(
        final_step(
            mirror_in,
            sample_part,
            keep_row,
            came_row,
            own_col,
            incoming,
            omega_blocks,
            0.5 / total_samples,
        )
    )


def solution(mesh):
    in_specs = (P("vars", "samp"), P("vars", None, None, None), P("vars", None))
    out_specs = (P("vars", None, "samp", None), P("vars", None, "samp", None))
    return jax.shard_map(
        step_on_device, mesh=mesh, in_specs=in_specs, out_specs=out_specs, check_vma=False
    )
```
